256 devices in a mesh: sub: 64 (over z, x, core), slab: 4 (over y).
Axes of the slice: x: 4, y: 4, z: 8, core: 2. Of those that a mesh axis runs over, the one named last changes fastest.
Arguments:
- residual: float32 [64, 4, 128, 1024], P('sub', 'slab'), may hold values from -6 to 6
- inverse_slab: float32 [64, 4, 1024, 1024], P('sub', 'slab'), may hold values from -1 to 2, as said below
- diagonal: float32 [64, 4, 1024], P('sub', 'slab'), may hold values from 0.2 to 0.6
- primal_index: int32 [64, 4, 32], P('sub', 'slab'), may hold values from 0 to 1023
- coarse_map: int32 [64, 32], P('sub'), may hold values from 0 to 1023
- schur_small: float32 [64, 32, 32], P('sub'), may hold values from -1 to 2, as said below
- constraint_basis: float32 [64, 4, 32, 1024], P('sub', 'slab'), may hold values from -0.75 to 0.75
- coarse_basis: float32 [64, 4, 32, 1024], P('sub', 'slab'), may hold values from -0.75 to 0.75
- coarse_inverse: float32 [1024, 1024], P(None, 'sub'), may hold values from -1 to 2, as said below
Outputs:
- preconditioned: float32 [64, 4, 128, 1024], P('sub', 'slab')
The draws below stay inside these ranges and needn't reach their ends.
Inputs may be any that keep to these rules, and one draw needn't show every extreme that they name: `inverse_slab`: A diagonal near 0.5 with full off-diagonal entries of moderate size. `schur_small`: A diagonal near 1 with full off-diagonal entries of moderate size. `coarse_inverse`: A diagonal near 1 with full off-diagonal entries of moderate size.
All inputs are finite; a program needn't handle non-finite values.
Results may differ from the reference program's by a relative error of at most 0.0001.
Values sent between devices are 32-bit elements; how exact they have to be, the bound alone decides.
A program may use at most 64 MiB of HBM per device.

```python
import math
import jax
import jax.numpy as jnp
from jax import lax

CXY = 32
RHS = 128
PRIM = 32
IFACE = 1024
SUBS = 64
SLABS = 4
NCOARSE = 1024


def dominant(key, leading, order, spread):
    shape = leading + (order, order)
    noise = jnp.clip(jax.random.normal(key, shape, jnp.float32), -4.0, 4.0)
    return jnp.eye(order, dtype=jnp.float32) + spread * noise / math.sqrt(order)


def draw_inverse_slab(key, part):
    return 0.5 * dominant(jax.random.fold_in(key, 11), (SUBS, SLABS), CXY * CXY, 0.6)


def draw_schur_small(key, part):
    return dominant(jax.random.fold_in(key, 23), (SUBS,), PRIM, 0.6)


def draw_coarse_inverse(key, part):
    return dominant(jax.random.fold_in(key, 37), (), NCOARSE, 0.6)


def with_ends(entries, stream_key, low, top_value):
    extent = entries.shape
    spot = [jax.random.randint(jax.random.fold_in(stream_key, axis), (), 0, extent[axis]) for axis in range(len(extent))]
    entries = entries.at[tuple(spot)].set(low)
    longest = extent.index(max(extent))
    spot[longest] = (spot[longest] + 1) % extent[longest]
    return entries.at[tuple(spot)].set(top_value)


def level_of(own_key, shape, pieces, smallest, high):
    gain, own = 1.0, jax.random.fold_in(own_key, 6)
    for axis_at, parts in pieces:
        draws = jnp.exp(jax.random.uniform(jax.random.fold_in(own, axis_at), (parts,), jnp.float32, smallest / len(pieces), high / len(pieces)))
        gain = gain * jnp.repeat(draws, shape[axis_at] // parts).reshape([-1 if axis == axis_at else 1 for axis in range(len(shape))])
    return gain


def normal_values(key, dims, scale, most, shards=(), kind=jnp.bfloat16):
    values = scale * jax.random.normal(key, dims, jnp.float32)
    if shards:
        values = values * level_of(key, dims, shards, -0.22, 0.18)
    return jnp.clip(values, -most, most).astype(kind)


def setup_inputs(seed: int = 0) -> dict:
    seeds = jax.random.split(jax.random.key(seed), 10)
    residual = normal_values(seeds[0], (SUBS, SLABS, RHS, IFACE), 1.0, 6.0, ((0, 64), (1, 4)), jnp.float32)
    inverse_slab = draw_inverse_slab(jax.random.fold_in(seeds[9], 71), 0)
    diagonal = jnp.clip(0.2 + 0.400000021 * jax.random.uniform(seeds[2], (SUBS, SLABS, IFACE), jnp.float32) ** level_of(seeds[2], (SUBS, SLABS, IFACE), ((0, 64), (1, 4)), -0.2, 0.2), 0.2, 0.6)
    primal_index = with_ends(jax.random.randint(seeds[3], (SUBS, SLABS, PRIM), 0, IFACE), jax.random.fold_in(seeds[3], 1), 0, IFACE - 1).astype(jnp.int32)
    coarse_map = with_ends(jax.random.randint(seeds[4], (SUBS, PRIM), 0, NCOARSE), jax.random.fold_in(seeds[4], 1), 0, NCOARSE - 1).astype(jnp.int32)
    schur_small = draw_schur_small(jax.random.fold_in(seeds[9], 71), 0)
    constraint_basis = normal_values(seeds[6], (SUBS, SLABS, PRIM, IFACE), 0.05, 0.75, ((0, 64), (1, 4)), jnp.float32)
    coarse_basis = normal_values(seeds[7], (SUBS, SLABS, PRIM, IFACE), 0.05, 0.75, ((0, 64), (1, 4)), jnp.float32)
    coarse_inverse = draw_coarse_inverse(jax.random.fold_in(seeds[9], 71), 0)
    return dict(residual=residual, inverse_slab=inverse_slab, diagonal=diagonal, primal_index=primal_index, coarse_map=coarse_map, schur_small=schur_small, constraint_basis=constraint_basis, coarse_basis=coarse_basis, coarse_inverse=coarse_inverse)


highest = lax.Precision.HIGHEST


def slab_times(vector, matrix):
    return jnp.einsum('srw,swv->srv', vector, matrix, precision=highest)


def apply_once(vector, inverse_slab, primal_index, coarse_map, schur_small, constraint_basis, coarse_basis, coarse_inverse):
    forward = []
    carried = jnp.zeros_like(vector[:, 0])
    for level in range(SLABS):
        carried = slab_times(vector[:, level] + carried, inverse_slab[:, level])
        forward.append(carried)
    backward = [None] * SLABS
    carried = jnp.zeros_like(vector[:, 0])
    for level in reversed(range(SLABS)):
        carried = forward[level] + slab_times(carried, inverse_slab[:, level])
        backward[level] = carried
    neumann = jnp.stack(backward, axis=1)
    picks = jnp.take_along_axis(neumann, primal_index[:, :, None, :].astype(jnp.int32), axis=3)
    primal = jnp.sum(picks, axis=1)
    multiplier = jnp.einsum('srp,spq->srq', primal, schur_small, precision=highest)
    constrained = neumann - jnp.einsum('srp,skpw->skrw', multiplier, constraint_basis, precision=highest)
    onehot = (coarse_map[:, :, None] == jnp.arange(NCOARSE, dtype=jnp.int32)[None, None, :]).astype(jnp.float32)
    coarse_rhs = jnp.einsum('srp,spn->rn', primal, onehot, precision=highest)
    coarse_sol = jnp.dot(coarse_rhs, coarse_inverse, precision=highest)
    picked = jnp.einsum('rn,spn->srp', coarse_sol, onehot, precision=highest)
    return constrained + jnp.einsum('srp,skpw->skrw', picked, coarse_basis, precision=highest)


def reference(residual, inverse_slab, diagonal, primal_index, coarse_map, schur_small, constraint_basis, coarse_basis, coarse_inverse):
    first_pass = apply_once(residual, inverse_slab, primal_index, coarse_map, schur_small, constraint_basis, coarse_basis, coarse_inverse)
    defect = residual - diagonal[:, :, None, :] * first_pass
    second_pass = apply_once(defect, inverse_slab, primal_index, coarse_map, schur_small, constraint_basis, coarse_basis, coarse_inverse)
    return first_pass + second_pass
```

```python
import functools

import jax
import jax.numpy as jnp
from jax import lax
from jax.experimental import pallas as pl
from jax.experimental.pallas import tpu as pltpu
from jax.sharding import Mesh
from jax.sharding import PartitionSpec as P

SUB = ("z", "x", "core")
MESH = pl.DeviceIdType.MESH
F32 = jnp.float32
BF16 = jnp.bfloat16

RHS = 128
IFACE = 1024
PRIM = 32
EXTRA = 2 * PRIM
MAIN = 16
SIDE = 32
NMAIN = RHS // MAIN
NSIDE = EXTRA // SIDE
BLOCK = 40


def split(value):
    high = value.astype(BF16)
    return high, (value - high.astype(F32)).astype(BF16)


def dot(left, right):
    return jnp.dot(left, right, preferred_element_type=F32)


def dot_t(left, right):
    return lax.dot_general(left, right, (((1,), (1,)), ((), ())), preferred_element_type=F32)


def dot3(left, right):
    rows = left.shape[0]
    left_high, left_low = split(left)
    right_high, right_low = split(right)
    both = dot(jnp.concatenate([left_high, left_low], axis=0), right_high)
    return both[:rows] + both[rows:] + dot(left_high, right_low)


def column_of(row):
    eye = lax.broadcasted_iota(jnp.int32, (PRIM, PRIM), 0) == lax.broadcasted_iota(
        jnp.int32, (PRIM, PRIM), 1
    )
    return jnp.sum(jnp.where(eye, jnp.broadcast_to(row, (PRIM, PRIM)), 0.0), axis=1, keepdims=True)


def onehot_of(column, width):
    lanes = lax.broadcasted_iota(jnp.int32, (PRIM, width), 1).astype(F32)
    return jnp.where(lanes == column, 1.0, 0.0).astype(BF16)


def kernel(
    nz, nx,
    res_ref, g_ref, diag_ref, idx_ref, map_ref, schur_ref, cb_ref, cbas_ref, cinv_ref, out_ref,
    ghi, glo, vx, r1, f1, rb1, n1, x2, r2, f2, rb2, n2, w0, gs, es, ct, gp1, gp2, yp1, yk1, yp2, yk2,
    f1_s, f1_r, b1_s, b1_r, f2_s, f2_r, b2_s, b2_r,
    gx_s, gx_r, gz_s, gz_r, gc_s, gc_r, y_s, y_r,
):
    k = lax.axis_index("slab")
    z, x, core = lax.axis_index("z"), lax.axis_index("x"), lax.axis_index("core")
    slabs = 4

    barrier = pltpu.get_barrier_semaphore()
    for d in range(1, slabs):
        pl.semaphore_signal(barrier, inc=1, device_id={"slab": lax.rem(k + d, slabs)}, device_id_type=MESH)
    for d in range(1, nx):
        pl.semaphore_signal(barrier, inc=1, device_id={"x": lax.rem(x + d, nx)}, device_id_type=MESH)
    for d in range(1, nz):
        pl.semaphore_signal(barrier, inc=1, device_id={"z": lax.rem(z + d, nz)}, device_id_type=MESH)
    pl.semaphore_signal(barrier, inc=1, device_id={"core": 1 - core}, device_id_type=MESH)

    own = (core * nz + z) * nx + x

    @pl.loop(0, IFACE // 64)
    def _(i):
        rows = pl.ds(pl.multiple_of(i * 64, 64), 64)
        high, low = split(g_ref[rows, :])
        ghi[rows, :] = high
        glo[rows, :] = low

    vx[0:RHS, :] = res_ref[...]

    @pl.when(k == 0)
    def _():
        r1[...] = jnp.zeros_like(r1)

    map_row = map_ref[...]
    map_col = column_of(map_row.astype(F32))
    owner, inner = map_row >> 4, map_row & 15
    place = (((owner & 1) * nz + (owner >> 3)) * nx + ((owner >> 1) & 3)) * 16 + inner
    place_hot = onehot_of(column_of(place.astype(F32)), IFACE)
    read_hot = onehot_of(column_of(idx_ref[...].astype(F32)), IFACE)

    quarter = cinv_ref[pl.ds(pl.multiple_of(k * 256, 256), 256), :]
    turned = quarter.T
    gs[own, 0:16, :] = turned[:, 0:128]
    gs[own, 16:32, :] = turned[:, 128:256]
    lanes = lax.broadcasted_iota(jnp.int32, (PRIM, 128), 1)
    subl = lax.broadcasted_iota(jnp.int32, (PRIM, 128), 0)
    map_lane = jnp.sum(
        jnp.where(lanes - PRIM * x == subl, jnp.broadcast_to(map_col, (PRIM, 128)), 0.0), axis=0, keepdims=True
    )
    gs[own, 32:BLOCK, :] = jnp.broadcast_to(map_lane, (8, 128))

    w0[0:PRIM, :] = -dot3(schur_ref[...], cb_ref[...])
    w0[PRIM:EXTRA, :] = cbas_ref[...]
    vx[RHS : RHS + EXTRA, :] = w0[...] * diag_ref[...]

    pl.semaphore_wait(barrier, (slabs - 1) + (nx - 1) + (nz - 1) + 1)

    def remote(src, dst, send, recv, to):
        return pltpu.make_async_remote_copy(
            src_ref=src, dst_ref=dst, send_sem=send, recv_sem=recv, device_id=to, device_id_type=MESH
        )

    up = {"slab": lax.rem(k + 1, slabs)}
    down = {"slab": lax.rem(k + slabs - 1, slabs)}

    def gather_x(buf, n):
        return [
            remote(buf.at[own], buf.at[own], gx_s.at[n, d], gx_r.at[n, d], {"x": lax.rem(x + d, nx)})
            for d in range(1, nx)
        ]

    def gather_z(buf, n):
        part = pl.ds((core * nz + z) * nx, nx)
        return [
            remote(buf.at[part], buf.at[part], gz_s.at[n, d], gz_r.at[n, d], {"z": lax.rem(z + d, nz)})
            for d in range(1, nz)
        ]

    def gather_core(buf, n):
        part = pl.ds(core * nz * nx, nz * nx)
        return [remote(buf.at[part], buf.at[part], gc_s.at[n], gc_r.at[n], {"core": 1 - core})]

    def among_slabs(buf, part, n):
        return [
            remote(buf.at[part], buf.at[part], y_s.at[n, d], y_r.at[n, d], {"slab": lax.rem(k + d, slabs)})
            for d in range(1, slabs)
        ]

    def start(copies):
        for copy in copies:
            copy.start()

    def arrived(copies):
        for copy in copies:
            copy.wait_recv()

    def sent(copies):
        for copy in copies:
            copy.wait_send()

    setup_x, setup_z, setup_c = gather_x(gs, 0), gather_z(gs, 0), gather_core(gs, 0)
    one_x, one_z, one_c = gather_x(gp1, 1), gather_z(gp1, 1), gather_core(gp1, 1)
    two_x, two_z, two_c = gather_x(gp2, 2), gather_z(gp2, 2), gather_core(gp2, 2)
    ey = among_slabs(es, pl.ds(2 * k, 2), 0)
    py1 = among_slabs(yp1, pl.ds(k, 1), 1)
    ky1 = among_slabs(yk1, pl.ds(k, 1), 2)
    py2 = among_slabs(yp2, pl.ds(k, 1), 3)
    ky2 = among_slabs(yk2, pl.ds(k, 1), 4)

    def times_g(value):
        rows = value.shape[0]
        high, low = split(value)
        both = dot(jnp.concatenate([high, low], axis=0), ghi[...])
        return both[:rows] + both[rows:] + dot(high, glo[...])

    def main_chunk(i):
        return i, pl.ds(pl.multiple_of(i * MAIN, MAIN), MAIN)

    def side_chunk(i):
        return NMAIN + i, pl.ds(pl.multiple_of(RHS + i * SIDE, SIDE), SIDE)

    def f1_copy(sem, rows):
        return remote(f1.at[rows], r1.at[rows], f1_s.at[sem], f1_r.at[sem], up)

    def b1_copy(sem, rows):
        return remote(n1.at[rows], rb1.at[rows], b1_s.at[sem], b1_r.at[sem], down)

    def f2_copy(sem, rows):
        return remote(f2.at[rows], r2.at[rows], f2_s.at[sem], f2_r.at[sem], up)

    def b2_copy(sem, rows):
        return remote(n2.at[rows], rb2.at[rows], b2_s.at[sem], b2_r.at[sem], down)

    def forward_one(sem, rows):
        @pl.when(k > 0)
        def _():
            f1_copy(sem, rows).wait_recv()

        value = times_g(vx[rows, :] + r1[rows, :])
        f1[rows, :] = value

        @pl.when(k < slabs - 1)
        def _():
            f1_copy(sem, rows).start()

        @pl.when(k == slabs - 1)
        def _():
            n1[rows, :] = value
            b1_copy(sem, rows).start()

    def backward_one(sem, rows):
        @pl.when(k < slabs - 1)
        def _():
            b1_copy(sem, rows).wait_recv()
            n1[rows, :] = f1[rows, :] + times_g(rb1[rows, :])

            @pl.when(k > 0)
            def _():
                b1_copy(sem, rows).start()

    def forward_two(sem, rows):
        @pl.when(k > 0)
        def _():
            f2_copy(sem, rows).wait_recv()
            value = times_g(x2[rows, :] + r2[rows, :])
            f2[rows, :] = value

            @pl.when(k < slabs - 1)
            def _():
                f2_copy(sem, rows).start()

            @pl.when(k == slabs - 1)
            def _():
                n2[rows, :] = value
                b2_copy(sem, rows).start()

    def backward_two(sem, rows):
        @pl.when(k < slabs - 1)
        def _():
            b2_copy(sem, rows).wait_recv()
            n2[rows, :] = f2[rows, :] + times_g(rb2[rows, :])

            @pl.when(k > 0)
            def _():
                b2_copy(sem, rows).start()

    def over_main(step):
        @pl.loop(0, NMAIN)
        def _(i):
            step(*main_chunk(i))

    def over_side(step):
        @pl.loop(0, NSIDE)
        def _(i):
            step(*side_chunk(i))

    def between(sem, rows):
        backward_one(sem, rows)
        value = res_ref[rows, :] - diag_ref[...] * n1[rows, :]
        x2[rows, :] = value

        @pl.when(k == 0)
        def _():
            forward = times_g(value)
            f2[rows, :] = forward
            f2_copy(sem, rows).start()

    def setup_to_z():
        arrived(setup_x)
        start(setup_z)

    start(setup_x)

    @pl.when(k > 0)
    def _():
        setup_to_z()

    over_main(forward_one)

    @pl.when(k == 0)
    def _():
        setup_to_z()

    @pl.when(k != 2)
    def _():
        over_side(forward_one)

    over_main(between)

    @pl.when(k == 2)
    def _():
        over_side(forward_one)

    arrived(setup_z)
    start(setup_c)
    arrived(setup_c)
    for half in range(2):
        table = gs[:, 16 * half : 16 * half + 16, :].reshape(IFACE, 128)
        high, low = split(table)
        es[2 * k + half] = dot(place_hot, high) + dot(place_hot, low)
    start(ey)

    over_side(backward_one)

    def primal_of(ref):
        high, low = split(ref[...])
        return dot_t(read_hot, high) + dot_t(read_hot, low)

    primal_one = primal_of(n1)
    yp1[k] = primal_one[:, 0:RHS]
    gp1[own] = primal_one[:, 0:RHS]
    side_primal = primal_one[:, RHS : RHS + EXTRA]
    start(py1)
    start(one_x)

    arrived(ey)
    e_high, e_low = split(jnp.concatenate([es[b] for b in range(8)], axis=1))
    e_both = jnp.concatenate([e_high, e_low], axis=0)
    depth = lax.broadcasted_iota(jnp.int32, (IFACE, 256), 0).astype(F32)

    @pl.loop(0, nz * nx * 2 // 8)
    def _(g):
        first = jnp.sum(gs[pl.ds(8 * g, 4), 32, :], axis=0, keepdims=True)
        second = jnp.sum(gs[pl.ds(8 * g + 4, 4), 32, :], axis=0, keepdims=True)
        wanted = jnp.concatenate([first, second], axis=1)
        hot = jnp.where(depth == wanted, 1.0, 0.0).astype(BF16)
        both = dot(e_both, hot)
        high, low = split(both[0:PRIM] + both[PRIM:])
        columns = pl.ds(pl.multiple_of(g * 256, 256), 256)
        ct[0:PRIM, columns] = high
        ct[PRIM:EXTRA, columns] = low

    def picked_of(buf):
        high, low = split(buf[...].reshape(nz * nx * 2 * PRIM, RHS))
        both = dot(ct[...], high)
        return both[0:PRIM] + both[PRIM:] + dot(ct[0:PRIM, :], low)

    arrived(one_x)
    start(one_z)

    over_main(forward_two)

    arrived(one_z)
    start(one_c)
    arrived(one_c)
    yk1[k] = picked_of(gp1)
    start(ky1)

    over_main(backward_two)

    arrived(py1)
    arrived(ky1)
    u1 = jnp.concatenate([jnp.sum(yp1[...], axis=0), jnp.sum(yk1[...], axis=0)], axis=0)
    primal_two = primal_of(n2) - dot3(side_primal, u1)
    yp2[k] = primal_two
    gp2[own] = primal_two
    start(two_x)
    start(py2)
    arrived(two_x)
    start(two_z)
    arrived(two_z)
    start(two_c)
    arrived(two_c)
    yk2[k] = picked_of(gp2)
    start(ky2)
    arrived(py2)
    arrived(ky2)
    u2 = jnp.concatenate([jnp.sum(yp2[...], axis=0), jnp.sum(yk2[...], axis=0)], axis=0)
    weights = jnp.concatenate([u1, u1 + u2], axis=0).T
    base = jnp.concatenate([-n1[RHS : RHS + EXTRA, :], w0[...]], axis=0)
    out_ref[...] = n1[0:RHS, :] + n2[...] + dot3(weights, base)

    for copies in (setup_x, setup_z, setup_c, one_x, one_z, one_c, two_x, two_z, two_c, ey, py1, ky1, py2, ky2):
        sent(copies)

    def sent_chunk(first):
        def step(sem, rows):
            @pl.when(k < slabs - 1)
            def _():
                (f1_copy if first else f2_copy)(sem, rows).wait_send()

            @pl.when(k > 0)
            def _():
                (b1_copy if first else b2_copy)(sem, rows).wait_send()

        return step

    over_main(sent_chunk(True))
    over_side(sent_chunk(True))
    over_main(sent_chunk(False))


def on_device(nz, nx, residual, inverse_slab, diagonal, primal_index, coarse_map, schur, basis_one, basis_two, cinv):
    subs = nz * nx * 2
    dma = pltpu.SemaphoreType.DMA
    vmem = pl.BlockSpec(memory_space=pltpu.VMEM)
    wide = lambda rows, kind=F32: pltpu.VMEM((rows, IFACE), kind)
    out = pl.pallas_call(
        functools.partial(kernel, nz, nx),
        out_shape=jax.ShapeDtypeStruct((RHS, IFACE), F32),
        in_specs=[vmem] * 9,
        out_specs=vmem,
        scratch_shapes=[
            wide(IFACE, BF16), wide(IFACE, BF16),
            *[wide(RHS + EXTRA)] * 5,
            *[wide(RHS)] * 5,
            wide(EXTRA),
            pltpu.VMEM((subs, BLOCK, 128), F32),
            pltpu.VMEM((8, PRIM, 128), F32),
            pltpu.VMEM((EXTRA, subs * PRIM), BF16),
            *[pltpu.VMEM((subs, PRIM, RHS), F32)] * 2,
            *[pltpu.VMEM((4, PRIM, RHS), F32)] * 4,
            *[dma((NMAIN + NSIDE,))] * 4,
            *[dma((NMAIN,))] * 4,
            dma((3, nx)), dma((3, nx)), dma((3, nz)), dma((3, nz)), dma((3,)), dma((3,)),
            dma((5, 4)), dma((5, 4)),
        ],
        compiler_params=pltpu.CompilerParams(
            collective_id=0, has_side_effects=True, vmem_limit_bytes=56 * 2**20
        ),
    )(
        residual[0, 0], inverse_slab[0, 0], diagonal[0], primal_index[0], coarse_map, schur[0],
        basis_one[0, 0], basis_two[0, 0], cinv,
    )
    return out[None, None]


def solution(mesh):
    nz, nx = 8, 4
    torus = Mesh(mesh.devices.reshape(nz, nx, 2, mesh.shape["slab"]), (*SUB, "slab"))
    in_specs = (
        P(SUB, "slab", None, None),
        P(SUB, "slab", None, None),
        P(SUB, "slab", None),
        P(SUB, "slab", None),
        P(SUB, None),
        P(SUB, None, None),
        P(SUB, "slab", None, None),
        P(SUB, "slab", None, None),
        P(None, SUB),
    )
    return jax.shard_map(
        functools.partial(on_device, nz, nx),
        mesh=torus,
        in_specs=in_specs,
        out_specs=P(SUB, "slab", None, None),
        check_vma=False,
    )
```

```python
import functools

import jax
import jax.numpy as jnp
from jax import lax
from jax.experimental import pallas as pl
from jax.experimental.pallas import tpu as pltpu
from jax.sharding import Mesh
from jax.sharding import PartitionSpec as P

SUB = ("z", "x", "core")
MESH = pl.DeviceIdType.MESH
F32 = jnp.float32
BF16 = jnp.bfloat16

RHS = 128
IFACE = 1024
PRIM = 32
EXTRA = 2 * PRIM
SLABS = 4
MAIN = 16
SIDE = 32
NMAIN = RHS // MAIN
NSIDE = EXTRA // SIDE
BLOCK = 40
PIECES = 8


def split(value):
    high = value.astype(BF16)
    return high, (value - high.astype(F32)).astype(BF16)


def dot(left, right):
    return jnp.dot(left, right, preferred_element_type=F32)


def dot_t(left, right):
    return lax.dot_general(left, right, (((1,), (1,)), ((), ())), preferred_element_type=F32)


def three(left, right, times):
    rows = left[0].shape[0]
    both = times(jnp.concatenate(left, axis=0), right[0])
    return both[:rows] + both[rows:] + times(left[0], right[1])


def dot3(left, right):
    return three(split(left), split(right), dot)


def column_of(row):
    eye = lax.broadcasted_iota(jnp.int32, (PRIM, PRIM), 0) == lax.broadcasted_iota(
        jnp.int32, (PRIM, PRIM), 1
    )
    return jnp.sum(jnp.where(eye, jnp.broadcast_to(row, (PRIM, PRIM)), 0.0), axis=1, keepdims=True)


def onehot_of(column, width):
    lanes = lax.broadcasted_iota(jnp.int32, (PRIM, width), 1).astype(F32)
    return jnp.where(lanes == column, 1.0, 0.0).astype(BF16)


def moved(tile, source, target):
    shift = 32 * (target - source) % 128
    return pltpu.roll(tile, shift, 1) if shift else tile


def groups_of(pieces):
    group = lax.broadcasted_iota(jnp.int32, (8, 128), 1) // 32
    total = jnp.zeros((8, 128), F32)
    for target, parts in enumerate(pieces):
        value = sum(moved(tile, source, target) for tile, source in parts)
        total = jnp.where(group == target, value, total)
    return total


def folded(tiles):
    return [groups_of([[(tiles[q], t)] for q in range(4)]) for t in range(4)]


def kernel(
    nz, nx,
    res_hbm, g_hbm, cb_hbm, cbas_hbm, diag_ref, idx_ref, map_ref, schur_ref, cinv_ref, out_ref,
    g, cb, ghi, glo, vx, r1, f1, rb1, n1, x2, r2, f2, rb2, n2, w0,
    ta, tu, tr, tk, td, hot, gs, ms, es, ch, cl, pf, ps, gp, ag, u1s, xys,
    in_s, f1_s, f1_r, b1_s, b1_r, f2_s, f2_r, b2_s, b2_r, t_s, t_r,
    gx_s, gx_r, gz_s, gz_r, gc_s, gc_r, y_s, y_r,
):
    k = lax.axis_index("slab")
    z, x, core = lax.axis_index("z"), lax.axis_index("x"), lax.axis_index("core")
    blocks = 2 * nx * nz

    piece = IFACE // PIECES
    loads = [
        pltpu.make_async_copy(g_hbm.at[pl.ds(i * piece, piece)], g.at[pl.ds(i * piece, piece)], in_s.at[i])
        for i in range(PIECES)
    ]
    load_res = pltpu.make_async_copy(res_hbm, vx.at[pl.ds(0, RHS)], in_s.at[PIECES])
    load_cb = pltpu.make_async_copy(cb_hbm, cb, in_s.at[PIECES + 1])
    load_cbas = pltpu.make_async_copy(cbas_hbm, w0.at[pl.ds(PRIM, PRIM)], in_s.at[PIECES + 2])
    for copy in (*loads, load_res, load_cb, load_cbas):
        copy.start()

    barrier = pltpu.get_barrier_semaphore()
    for d in range(1, nz):
        pl.semaphore_signal(barrier, inc=1, device_id={"z": lax.rem(z + d, nz)}, device_id_type=MESH)
    for d in range(1, SLABS):
        pl.semaphore_signal(barrier, inc=1, device_id={"slab": lax.rem(k + d, SLABS)}, device_id_type=MESH)
    for d in range(1, nx):
        pl.semaphore_signal(barrier, inc=1, device_id={"x": lax.rem(x + d, nx)}, device_id_type=MESH)
    pl.semaphore_signal(barrier, inc=1, device_id={"core": 1 - core}, device_id_type=MESH)

    own = (core * nx + x) * nz + z

    @pl.when(k == 0)
    def _():
        r1[...] = jnp.zeros_like(r1)
        tr[...] = jnp.zeros_like(tr)

    map_row = map_ref[...]
    map_col = column_of(map_row.astype(F32))
    owner, inner = map_row >> 4, map_row & 15
    place = (((owner & 1) * nx + ((owner >> 1) & 3)) * nz + (owner >> 3)) * 16 + inner
    hot[0:PRIM, :] = onehot_of(column_of(place.astype(F32)), IFACE)
    hot[PRIM:EXTRA, :] = onehot_of(column_of(idx_ref[...].astype(F32)), IFACE)

    quarter = pl.ds(pl.multiple_of(k * 256, 256), 256)
    gs[own, 0:16, :] = cinv_ref[:, quarter][:, 0:128]
    gs[own, 16:32, :] = cinv_ref[:, quarter][:, 128:256]
    lanes = lax.broadcasted_iota(jnp.int32, (PRIM, 128), 1)
    subl = lax.broadcasted_iota(jnp.int32, (PRIM, 128), 0)
    spread = jnp.where(lanes - 8 * lax.rem(own, 16) == subl % 8, jnp.broadcast_to(map_col, (PRIM, 128)), 0.0)
    for t in range(4):
        gs[own, 32 + t : 33 + t, :] = jnp.sum(spread[8 * t : 8 * t + 8], axis=0, keepdims=True)
    gs[own, 36:40, :] = jnp.zeros((4, 128), F32)

    load_cb.wait()
    load_cbas.wait()
    w0[0:PRIM, :] = -dot3(schur_ref[...], cb[...])
    vx[RHS : RHS + EXTRA, :] = w0[...] * diag_ref[...]

    for i in range(PIECES):
        loads[i].wait()

        @pl.loop(0, piece // 64)
        def _(j):
            rows = pl.ds(pl.multiple_of(i * piece + j * 64, 64), 64)
            high, low = split(g[rows, :])
            ghi[rows, :] = high
            glo[rows, :] = low

    load_res.wait()
    pl.semaphore_wait(barrier, (SLABS - 1) + (nx - 1) + (nz - 1) + 1)

    def remote(src, dst, send, recv, to):
        return pltpu.make_async_remote_copy(
            src_ref=src, dst_ref=dst, send_sem=send, recv_sem=recv, device_id=to, device_id_type=MESH
        )

    up = {"slab": lax.rem(k + 1, SLABS)}
    down = {"slab": lax.rem(k + SLABS - 1, SLABS)}

    def gather_z(buf, n):
        return [
            remote(buf.at[own], buf.at[own], gz_s.at[n, d], gz_r.at[n, d], {"z": lax.rem(z + d, nz)})
            for d in range(1, nz)
        ]

    def gather_x(buf, n):
        part = pl.ds((core * nx + x) * nz, nz)
        return [
            remote(buf.at[part], buf.at[part], gx_s.at[n, d], gx_r.at[n, d], {"x": lax.rem(x + d, nx)})
            for d in range(1, nx)
        ]

    def gather_core(buf, n):
        part = pl.ds(core * nx * nz, nx * nz)
        return [remote(buf.at[part], buf.at[part], gc_s.at[n], gc_r.at[n], {"core": 1 - core})]

    def to_slabs(copy_of, n):
        made = []
        for d in range(1, SLABS):
            other = lax.rem(k + d, SLABS)
            src, dst = copy_of(other)
            made.append(remote(src, dst, y_s.at[n, d], y_r.at[n, d], {"slab": other}))
        return made

    def start(copies):
        for copy in copies:
            copy.start()

    def arrived(copies):
        for copy in copies:
            copy.wait_recv()

    def sent(copies):
        for copy in copies:
            copy.wait_send()

    setup_z, setup_x, setup_c = gather_z(gs, 2), gather_x(gs, 2), gather_core(gs, 2)
    e_part = pl.ds(2 * k, 2)
    ey = to_slabs(lambda other: (es.at[e_part], es.at[e_part]), 4)
    coarse_z = [gather_z(gp.at[n], n) for n in range(2)]
    coarse_x = [gather_x(gp.at[n], n) for n in range(2)]
    coarse_c = [gather_core(gp.at[n], n) for n in range(2)]
    fold_y = [to_slabs(lambda other: (pf.at[n, other], ps.at[n, k]), 2 * n) for n in range(2)]
    back_y = [to_slabs(lambda other: (ag.at[n, k], ag.at[n, k]), 2 * n + 1) for n in range(2)]

    def times_g(value):
        return three(split(value), (ghi[...], glo[...]), dot)

    def times_g_turned(value):
        return three(split(value), (ghi[...], glo[...]), dot_t)

    def main_chunk(i):
        return i, pl.ds(pl.multiple_of(i * MAIN, MAIN), MAIN)

    def side_chunk(i):
        return NMAIN + i, pl.ds(pl.multiple_of(RHS + i * SIDE, SIDE), SIDE)

    def f1_copy(sem, rows):
        return remote(f1.at[rows], r1.at[rows], f1_s.at[sem], f1_r.at[sem], up)

    def b1_copy(sem, rows):
        return remote(n1.at[rows], rb1.at[rows], b1_s.at[sem], b1_r.at[sem], down)

    def f2_copy(sem, rows):
        return remote(f2.at[rows], r2.at[rows], f2_s.at[sem], f2_r.at[sem], up)

    def b2_copy(sem, rows):
        return remote(n2.at[rows], rb2.at[rows], b2_s.at[sem], b2_r.at[sem], down)

    def forward_one(sem, rows):
        @pl.when(k > 0)
        def _():
            f1_copy(sem, rows).wait_recv()

        value = times_g(vx[rows, :] + r1[rows, :])
        f1[rows, :] = value

        @pl.when(k < SLABS - 1)
        def _():
            f1_copy(sem, rows).start()

        @pl.when(k == SLABS - 1)
        def _():
            n1[rows, :] = value
            b1_copy(sem, rows).start()

    def backward_one(sem, rows):
        @pl.when(k < SLABS - 1)
        def _():
            b1_copy(sem, rows).wait_recv()
            n1[rows, :] = f1[rows, :] + times_g(rb1[rows, :])

            @pl.when(k > 0)
            def _():
                b1_copy(sem, rows).start()

    def between(sem, rows):
        backward_one(sem, rows)
        value = vx[rows, :] - diag_ref[...] * n1[rows, :]
        x2[rows, :] = value

        @pl.when(k == 0)
        def _():
            f2[rows, :] = times_g(value)
            f2_copy(sem, rows).start()

    def forward_two(sem, rows):
        @pl.when(k > 0)
        def _():
            f2_copy(sem, rows).wait_recv()
            value = times_g(x2[rows, :] + r2[rows, :])
            f2[rows, :] = value

            @pl.when(k < SLABS - 1)
            def _():
                f2_copy(sem, rows).start()

            @pl.when(k == SLABS - 1)
            def _():
                n2[rows, :] = value
                b2_copy(sem, rows).start()

    def backward_two(sem, rows):
        @pl.when(k < SLABS - 1)
        def _():
            b2_copy(sem, rows).wait_recv()
            n2[rows, :] = f2[rows, :] + times_g(rb2[rows, :])

            @pl.when(k > 0)
            def _():
                b2_copy(sem, rows).start()

    def over_main(step, hooks=()):
        @pl.loop(0, NMAIN)
        def _(i):
            step(*main_chunk(i))
            for act, places in hooks:
                due = functools.reduce(jnp.logical_or, [(k == slab) & (i == at) for slab, at in places.items()])
                pl.when(due)(act)

    def over_side(step):
        @pl.loop(0, NSIDE)
        def _(i):
            step(*side_chunk(i))

    def only(slabs, *acts):
        @pl.when(functools.reduce(jnp.logical_or, [k == slab for slab in slabs]))
        def _():
            for act in acts:
                act()

    side_forward = lambda: over_side(forward_one)
    side_backward = lambda: over_side(backward_one)

    turned_up = remote(tu, tr, t_s.at[0], t_r.at[0], up)
    turned_down = remote(tk, td, t_s.at[1], t_r.at[1], down)

    def adjoint_up():
        @pl.when(k > 0)
        def _():
            turned_up.wait_recv()

        value = hot[PRIM:EXTRA, :].astype(F32) + tr[...]
        ta[...] = value
        result = times_g_turned(value)

        @pl.when(k < SLABS - 1)
        def _():
            tu[...] = result
            turned_up.start()

        @pl.when(k == SLABS - 1)
        def _():
            tk[...] = result
            turned_down.start()

    def adjoint_down():
        turned_down.wait_recv()
        tk[...] = times_g_turned(ta[...] + td[...])

        @pl.when(k > 0)
        def _():
            turned_down.start()

    def setup_z_in():
        arrived(setup_z)
        start(setup_x)

    def setup_x_in():
        arrived(setup_x)
        start(setup_c)

    def setup_core_in():
        arrived(setup_c)
        for half in range(2):
            high, low = split(gs[:, 16 * half : 16 * half + 16, :].reshape(IFACE, 128))
            es[2 * k + half] = dot(hot[0:PRIM, :], high) + dot(hot[0:PRIM, :], low)
        start(ey)

    def coarse_operator():
        arrived(ey)
        for a in range(4):
            ms[a] = jnp.sum(gs[16 * a : 16 * a + 16, 32:40, :], axis=0)
        wide = jnp.concatenate([es[b] for b in range(8)], axis=1)
        both_e = jnp.concatenate(split(wide), axis=0)
        depth = lax.broadcasted_iota(jnp.int32, (IFACE, 256), 0).astype(F32)
        for half in range(2):

            @pl.loop(0, 4)
            def _(t):
                wanted = jnp.concatenate([ms[2 * half, pl.ds(t, 1), :], ms[2 * half + 1, pl.ds(t, 1), :]], axis=1)
                both = dot(both_e, jnp.where(depth == wanted, 1.0, 0.0).astype(BF16))
                high, low = split(both[0:PRIM] + both[PRIM:])
                rows = pl.ds(pl.multiple_of(t * PRIM, PRIM), PRIM)
                ch[rows, 256 * half : 256 * half + 256] = high
                cl[rows, 256 * half : 256 * half + 256] = low

    def give_primal(n, primal):
        tiles = folded([primal[8 * t : 8 * t + 8] for t in range(4)])
        for q in range(4):
            pf[n, q] = tiles[q]
        ps[n, k] = pf[n, k]
        start(fold_y[n])

    def primal_one():
        high, low = split(n1[0:RHS, :])
        reads = hot[PRIM:EXTRA, :]
        give_primal(0, dot_t(reads, high) + dot_t(reads, low))

    def solve_sum(n):
        arrived(fold_y[n])
        total = jnp.sum(ps[n], axis=0)
        gp[n, own] = total
        ag[n, k, 0:8, :] = total
        start(coarse_z[n])

    def solve_z(n):
        arrived(coarse_z[n])
        start(coarse_x[n])

    def solve_x(n):
        arrived(coarse_x[n])
        start(coarse_c[n])

    def solve_core(n):
        arrived(coarse_c[n])
        everyone = split(gp[n].reshape(blocks * 8, 128))
        product = three((ch[...], cl[...]), everyone, dot)
        ag[n, k, 8:16, :] = groups_of(
            [[(product[32 * t + 8 * target : 32 * t + 8 * target + 8], t) for t in range(4)] for target in range(4)]
        )
        start(back_y[n])

    def solved(n):
        arrived(back_y[n])
        tiles = [ag[n, q] for q in range(4)]
        return jnp.concatenate(
            [*folded([tile[0:8] for tile in tiles]), *folded([tile[8:16] for tile in tiles])], axis=0
        )

    def adjoint_products():
        turned = split(tk[...])
        xys[:, 0:RHS] = three(turned, split(x2[...]), dot_t)
        xys[:, RHS : RHS + EXTRA] = three(turned, split(vx[RHS : RHS + EXTRA, :]), dot_t)

    def solved_one():
        u1 = solved(0)
        u1s[...] = u1
        give_primal(1, xys[:, 0:RHS] - dot3(xys[:, RHS : RHS + EXTRA], u1))

    sum0, z0, x0, core0 = (functools.partial(act, 0) for act in (solve_sum, solve_z, solve_x, solve_core))
    sum1, z1, x1, core1 = (functools.partial(act, 1) for act in (solve_sum, solve_z, solve_x, solve_core))

    start(setup_z)
    only((2, 3), setup_z_in)
    over_main(forward_one, [(setup_z_in, {0: 6, 1: 2}), (setup_x_in, {2: 6, 3: 3}), (setup_core_in, {3: 5})])
    only((1,), setup_x_in)
    only((2,), setup_core_in)
    only((0, 1, 3), adjoint_up)
    only((1,), setup_core_in)
    only((0, 1), side_forward)
    only((0,), setup_x_in, setup_core_in)
    over_main(between, [(adjoint_up, {2: 5})])
    primal_one()
    only((3,), coarse_operator)
    only((2, 3), side_forward)
    only((2,), coarse_operator)
    only((3,), adjoint_products)
    over_main(
        forward_two,
        [(adjoint_down, {2: 1}), (sum0, {2: 4, 3: 0}), (adjoint_products, {2: 5}), (z0, {2: 7, 3: 3}), (x0, {3: 6})],
    )
    only((1,), sum0, adjoint_down, coarse_operator, z0, adjoint_products, x0, core0)
    only((0,), sum0, coarse_operator, z0, adjoint_down, adjoint_products, x0, core0, solved_one)
    only((3,), core0, solved_one)
    only((2,), side_backward)
    over_main(
        backward_two,
        [
            (x0, {2: 3}),
            (core0, {2: 4}),
            (solved_one, {1: 2, 2: 6}),
            (side_backward, {0: 6, 1: 3}),
            (sum1, {0: 2, 1: 4, 2: 7}),
            (z1, {0: 5, 1: 7}),
        ],
    )
    only((3,), sum1)
    only((2, 3), z1)
    u1 = u1s[...]
    weights = jnp.concatenate([u1, u1], axis=0).T
    base = jnp.concatenate([-n1[RHS : RHS + EXTRA, :], w0[...]], axis=0)
    out_ref[...] = n1[0:RHS, :] + n2[...] + dot3(weights, base)
    x1()
    core1()
    u2 = solved(1)
    weights = jnp.concatenate([u2, jnp.zeros_like(u2)], axis=0).T
    out_ref[...] += dot3(weights[:, 0:EXTRA], w0[...])

    for copies in (
        setup_z, setup_x, setup_c, ey, *coarse_z, *coarse_x, *coarse_c, *fold_y, *back_y,
    ):
        sent(copies)

    @pl.when(k < SLABS - 1)
    def _():
        turned_up.wait_send()

    @pl.when(k > 0)
    def _():
        turned_down.wait_send()

    def sent_chunk(first):
        def step(sem, rows):
            @pl.when(k < SLABS - 1)
            def _():
                (f1_copy if first else f2_copy)(sem, rows).wait_send()

            @pl.when(k > 0)
            def _():
                (b1_copy if first else b2_copy)(sem, rows).wait_send()

        return step

    over_main(sent_chunk(True))
    over_side(sent_chunk(True))
    over_main(sent_chunk(False))


def on_device(nz, nx, residual, inverse_slab, diagonal, primal_index, coarse_map, schur, basis_one, basis_two, cinv):
    blocks = nz * nx * 2
    dma = pltpu.SemaphoreType.DMA
    vmem = pl.BlockSpec(memory_space=pltpu.VMEM)
    hbm = pl.BlockSpec(memory_space=pl.ANY)
    wide = lambda rows, kind=F32: pltpu.VMEM((rows, IFACE), kind)
    out = pl.pallas_call(
        functools.partial(kernel, nz, nx),
        out_shape=jax.ShapeDtypeStruct((RHS, IFACE), F32),
        in_specs=[hbm] * 4 + [vmem] * 5,
        out_specs=vmem,
        scratch_shapes=[
            wide(IFACE), wide(PRIM), wide(IFACE, BF16), wide(IFACE, BF16),
            *[wide(RHS + EXTRA)] * 5,
            *[wide(RHS)] * 5,
            wide(EXTRA),
            *[wide(PRIM)] * 5,
            wide(EXTRA, BF16),
            pltpu.VMEM((blocks, BLOCK, 128), F32),
            pltpu.VMEM((4, 8, 128), F32),
            pltpu.VMEM((8, PRIM, 128), F32),
            *[pltpu.VMEM((128, blocks * 8), BF16)] * 2,
            *[pltpu.VMEM((2, 4, 8, 128), F32)] * 2,
            pltpu.VMEM((2, blocks, 8, 128), F32),
            pltpu.VMEM((2, 4, 16, 128), F32),
            pltpu.VMEM((EXTRA, RHS), F32),
            pltpu.VMEM((PRIM, RHS + EXTRA), F32),
            dma((PIECES + 3,)),
            *[dma((NMAIN + NSIDE,))] * 4,
            *[dma((NMAIN,))] * 4,
            dma((2,)), dma((2,)),
            dma((3, nx)), dma((3, nx)), dma((3, nz)), dma((3, nz)), dma((3,)), dma((3,)),
            dma((5, SLABS)), dma((5, SLABS)),
        ],
        compiler_params=pltpu.CompilerParams(
            collective_id=0, has_side_effects=True, vmem_limit_bytes=56 * 2**20
        ),
    )(
        residual[0, 0], inverse_slab[0, 0], basis_one[0, 0], basis_two[0, 0], diagonal[0], primal_index[0],
        coarse_map, schur[0], cinv.T,
    )
    return out[None, None]


def solution(mesh):
    nz, nx = 8, 4
    torus = Mesh(mesh.devices.reshape(nz, nx, 2, mesh.shape["slab"]), (*SUB, "slab"))
    in_specs = (
        P(SUB, "slab", None, None),
        P(SUB, "slab", None, None),
        P(SUB, "slab", None),
        P(SUB, "slab", None),
        P(SUB, None),
        P(SUB, None, None),
        P(SUB, "slab", None, None),
        P(SUB, "slab", None, None),
        P(None, SUB),
    )
    return jax.shard_map(
        functools.partial(on_device, nz, nx),
        mesh=torus,
        in_specs=in_specs,
        out_specs=P(SUB, "slab", None, None),
        check_vma=False,
    )
```

```python
import functools

import jax
import jax.numpy as jnp
from jax import lax
from jax.experimental import pallas as pl
from jax.experimental.pallas import tpu as pltpu
from jax.sharding import Mesh
from jax.sharding import PartitionSpec as P

SUB = ("z", "x", "core")
MESH = pl.DeviceIdType.MESH
F32 = jnp.float32
BF16 = jnp.bfloat16

RHS = 128
IFACE = 1024
PRIM = 32
EXTRA = 2 * PRIM
SLABS = 4
MAIN = 16
SIDE = 32
NMAIN = RHS // MAIN
NTURN = PRIM // MAIN
EARLY = 3
NSIDE = EXTRA // SIDE
BLOCK = 40
PIECES = 8


def split(value):
    high = value.astype(BF16)
    return high, (value - high.astype(F32)).astype(BF16)


def dot(left, right):
    return jnp.dot(left, right, preferred_element_type=F32)


def dot_t(left, right):
    return lax.dot_general(left, right, (((1,), (1,)), ((), ())), preferred_element_type=F32)


def three(left, right, times):
    rows = left[0].shape[0]
    both = times(jnp.concatenate(left, axis=0), right[0])
    return both[:rows] + both[rows:] + times(left[0], right[1])


def dot3(left, right):
    return three(split(left), split(right), dot)


def column_of(row):
    eye = lax.broadcasted_iota(jnp.int32, (PRIM, PRIM), 0) == lax.broadcasted_iota(
        jnp.int32, (PRIM, PRIM), 1
    )
    return jnp.sum(jnp.where(eye, jnp.broadcast_to(row, (PRIM, PRIM)), 0.0), axis=1, keepdims=True)


def onehot_of(column, width):
    lanes = lax.broadcasted_iota(jnp.int32, (PRIM, width), 1).astype(F32)
    return jnp.where(lanes == column, 1.0, 0.0).astype(BF16)


def moved(tile, source, target):
    shift = 32 * (target - source) % 128
    return pltpu.roll(tile, shift, 1) if shift else tile


def groups_of(pieces):
    group = lax.broadcasted_iota(jnp.int32, (8, 128), 1) // 32
    total = jnp.zeros((8, 128), F32)
    for target, parts in enumerate(pieces):
        value = sum(moved(tile, source, target) for tile, source in parts)
        total = jnp.where(group == target, value, total)
    return total


def folded(tiles):
    return [groups_of([[(tiles[q], t)] for q in range(4)]) for t in range(4)]


def kernel(
    nz, nx,
    res_hbm, g_hbm, cb_hbm, cbas_hbm, diag_hbm, idx_hbm, map_hbm, schur_hbm, cinv_hbm, out_ref,
    diag_ref, idx_ref, map_ref, schur_ref, cinv_ref, g, cb, ghi, glo, vx, r1, f1, rb1, n1, x2, r2, f2, rb2, n2, w0,
    ta, tu, tr, tk, td, hot, gs, ms, es, ch, cl, pf, ps, gp, ag, u1s, xys,
    in_s, f1_s, f1_r, b1_s, b1_r, f2_s, f2_r, b2_s, b2_r, t_s, t_r,
    gx_s, gx_r, gz_s, gz_r, gp_s, gp_r, gc_s, gc_r, y_s, y_r,
):
    k = lax.axis_index("slab")
    z, x, core = lax.axis_index("z"), lax.axis_index("x"), lax.axis_index("core")
    blocks = 2 * nx * nz

    piece = IFACE // PIECES
    loads = [
        pltpu.make_async_copy(g_hbm.at[pl.ds(i * piece, piece)], g.at[pl.ds(i * piece, piece)], in_s.at[i])
        for i in range(PIECES)
    ]
    small = [
        pltpu.make_async_copy(src, dst, in_s.at[PIECES + 3 + i])
        for i, (src, dst) in enumerate(
            [(map_hbm, map_ref), (idx_hbm, idx_ref), (cinv_hbm, cinv_ref), (diag_hbm, diag_ref), (schur_hbm, schur_ref)]
        )
    ]
    load_res = pltpu.make_async_copy(res_hbm, vx.at[pl.ds(0, RHS)], in_s.at[PIECES])
    load_cb = pltpu.make_async_copy(cb_hbm, cb, in_s.at[PIECES + 1])
    load_cbas = pltpu.make_async_copy(cbas_hbm, w0.at[pl.ds(PRIM, PRIM)], in_s.at[PIECES + 2])
    for copy in (*small[:3], *loads, load_res, *small[3:], load_cb, load_cbas):
        copy.start()

    barrier = pltpu.get_barrier_semaphore()
    plane = [
        {"z": lax.rem(z + dz, nz), "x": lax.rem(x + dx, nx)}
        for dz in sorted(range(nz), key=lambda d: -min(d, nz - d))
        for dx in sorted(range(nx), key=lambda d: -min(d, nx - d))
        if dz or dx
    ]
    for other in plane:
        pl.semaphore_signal(barrier, inc=1, device_id=other, device_id_type=MESH)
    for d in range(1, SLABS):
        pl.semaphore_signal(barrier, inc=1, device_id={"slab": lax.rem(k + d, SLABS)}, device_id_type=MESH)
    pl.semaphore_signal(barrier, inc=1, device_id={"core": 1 - core}, device_id_type=MESH)

    own = (core * nx + x) * nz + z

    @pl.when(k == 0)
    def _():
        r1[...] = jnp.zeros_like(r1)
        tr[...] = jnp.zeros_like(tr)

    for copy in small[:3]:
        copy.wait()
    map_row = map_ref[...]
    map_col = column_of(map_row.astype(F32))
    owner, inner = map_row >> 4, map_row & 15
    place = (((owner & 1) * nx + ((owner >> 1) & 3)) * nz + (owner >> 3)) * 16 + inner
    hot[0:PRIM, :] = onehot_of(column_of(place.astype(F32)), IFACE)
    hot[PRIM:EXTRA, :] = onehot_of(column_of(idx_ref[...].astype(F32)), IFACE)

    quarter = pl.ds(pl.multiple_of(k * 256, 256), 256)
    gs[own, 0:16, :] = cinv_ref[:, quarter][:, 0:128]
    gs[own, 16:32, :] = cinv_ref[:, quarter][:, 128:256]
    lanes = lax.broadcasted_iota(jnp.int32, (PRIM, 128), 1)
    subl = lax.broadcasted_iota(jnp.int32, (PRIM, 128), 0)
    spread = jnp.where(lanes - 8 * lax.rem(own, 16) == subl % 8, jnp.broadcast_to(map_col, (PRIM, 128)), 0.0)
    for t in range(4):
        gs[own, 32 + t : 33 + t, :] = jnp.sum(spread[8 * t : 8 * t + 8], axis=0, keepdims=True)
    gs[own, 36:40, :] = jnp.zeros((4, 128), F32)

    def bases():
        for copy in (*small[3:], load_cb, load_cbas):
            copy.wait()
        w0[0:PRIM, :] = -dot3(schur_ref[...], cb[...])
        vx[RHS : RHS + EXTRA, :] = w0[...] * diag_ref[...]

    for i in range(PIECES):
        loads[i].wait()

        @pl.loop(0, piece // 64)
        def _(j):
            rows = pl.ds(pl.multiple_of(i * piece + j * 64, 64), 64)
            high, low = split(g[rows, :])
            ghi[rows, :] = high
            glo[rows, :] = low

    load_res.wait()
    pl.semaphore_wait(barrier, (SLABS - 1) + len(plane) + 1)

    def remote(src, dst, send, recv, to):
        return pltpu.make_async_remote_copy(
            src_ref=src, dst_ref=dst, send_sem=send, recv_sem=recv, device_id=to, device_id_type=MESH
        )

    up = {"slab": lax.rem(k + 1, SLABS)}
    down = {"slab": lax.rem(k + SLABS - 1, SLABS)}

    def gather_z(buf):
        return [
            remote(buf.at[own], buf.at[own], gz_s.at[d], gz_r.at[d], {"z": lax.rem(z + d, nz)})
            for d in range(1, nz)
        ]

    def gather_x(buf):
        part = pl.ds((core * nx + x) * nz, nz)
        return [
            remote(buf.at[part], buf.at[part], gx_s.at[d], gx_r.at[d], {"x": lax.rem(x + d, nx)})
            for d in range(1, nx)
        ]

    def gather_plane(buf, n):
        return [
            remote(buf.at[own], buf.at[own], gp_s.at[n, d], gp_r.at[n, d], other) for d, other in enumerate(plane)
        ]

    def gather_core(buf, n):
        part = pl.ds(core * nx * nz, nx * nz)
        return [remote(buf.at[part], buf.at[part], gc_s.at[n], gc_r.at[n], {"core": 1 - core})]

    def to_slabs(copy_of, n):
        made = []
        for d in range(1, SLABS):
            other = lax.rem(k + d, SLABS)
            src, dst = copy_of(other)
            made.append(remote(src, dst, y_s.at[n, d], y_r.at[n, d], {"slab": other}))
        return made

    def start(copies):
        for copy in copies:
            copy.start()

    def arrived(copies):
        for copy in copies:
            copy.wait_recv()

    def sent(copies):
        for copy in copies:
            copy.wait_send()

    setup_z, setup_x, setup_c = gather_z(gs), gather_x(gs), gather_core(gs, 2)
    e_part = pl.ds(2 * k, 2)
    ey = to_slabs(lambda other: (es.at[e_part], es.at[e_part]), 4)
    coarse_p = [gather_plane(gp.at[n], n) for n in range(2)]
    coarse_c = [gather_core(gp.at[n], n) for n in range(2)]
    fold_y = [to_slabs(lambda other: (pf.at[n, other], ps.at[n, k]), 2 * n) for n in range(2)]
    back_y = [to_slabs(lambda other: (ag.at[n, k], ag.at[n, k]), 2 * n + 1) for n in range(2)]

    def times_g(value):
        return three(split(value), (ghi[...], glo[...]), dot)

    def times_g_turned(value):
        return three(split(value), (ghi[...], glo[...]), dot_t)

    def main_chunk(i):
        return i, pl.ds(pl.multiple_of(i * MAIN, MAIN), MAIN)

    def side_chunk(i):
        return NMAIN + i, pl.ds(pl.multiple_of(RHS + i * SIDE, SIDE), SIDE)

    def f1_copy(sem, rows):
        return remote(f1.at[rows], r1.at[rows], f1_s.at[sem], f1_r.at[sem], up)

    def b1_copy(sem, rows):
        return remote(n1.at[rows], rb1.at[rows], b1_s.at[sem], b1_r.at[sem], down)

    def f2_copy(sem, rows):
        return remote(f2.at[rows], r2.at[rows], f2_s.at[sem], f2_r.at[sem], up)

    def b2_copy(sem, rows):
        return remote(n2.at[rows], rb2.at[rows], b2_s.at[sem], b2_r.at[sem], down)

    def forward_one(sem, rows):
        @pl.when(k > 0)
        def _():
            f1_copy(sem, rows).wait_recv()

        value = times_g(vx[rows, :] + r1[rows, :])
        f1[rows, :] = value

        @pl.when(k < SLABS - 1)
        def _():
            f1_copy(sem, rows).start()

        @pl.when(k == SLABS - 1)
        def _():
            n1[rows, :] = value
            b1_copy(sem, rows).start()

    def backward_one(sem, rows):
        @pl.when(k < SLABS - 1)
        def _():
            b1_copy(sem, rows).wait_recv()
            n1[rows, :] = f1[rows, :] + times_g(rb1[rows, :])

            @pl.when(k > 0)
            def _():
                b1_copy(sem, rows).start()

    def between(sem, rows):
        backward_one(sem, rows)
        value = vx[rows, :] - diag_ref[...] * n1[rows, :]
        x2[rows, :] = value

        @pl.when(k == 0)
        def _():
            f2[rows, :] = times_g(value)
            f2_copy(sem, rows).start()

    def forward_two(sem, rows):
        @pl.when(k > 0)
        def _():
            f2_copy(sem, rows).wait_recv()
            value = times_g(x2[rows, :] + r2[rows, :])
            f2[rows, :] = value

            @pl.when(k < SLABS - 1)
            def _():
                f2_copy(sem, rows).start()

            @pl.when(k == SLABS - 1)
            def _():
                n2[rows, :] = value
                b2_copy(sem, rows).start()

    def backward_two(sem, rows):
        @pl.when(k < SLABS - 1)
        def _():
            b2_copy(sem, rows).wait_recv()
            n2[rows, :] = f2[rows, :] + times_g(rb2[rows, :])

            @pl.when(k > 0)
            def _():
                b2_copy(sem, rows).start()

    def over_main(step, hooks=()):
        @pl.loop(0, NMAIN)
        def _(i):
            step(*main_chunk(i))
            for act, places in hooks:
                due = functools.reduce(
                    jnp.logical_or, [(k == slab) & (i == at) for slab, spots in places.items() for at in spots]
                )
                done = sum(jnp.where((k == slab) & (i > at), 1, 0) for slab, spots in places.items() for at in spots)

                @pl.when(due)
                def _():
                    act(done)

    def over_side(step):
        @pl.loop(0, NSIDE)
        def _(i):
            step(*side_chunk(i))

    def only(slabs, *acts):
        @pl.when(functools.reduce(jnp.logical_or, [k == slab for slab in slabs]))
        def _():
            for act in acts:
                act()

    def once(act, *args):
        return lambda *_: act(*args)

    def side_forward(i):
        forward_one(*side_chunk(i))

    def side_backward(i):
        backward_one(*side_chunk(i))

    def all_side_forward():
        over_side(forward_one)

    def all_side_backward():
        over_side(backward_one)

    def turned_up(i):
        rows = pl.ds(pl.multiple_of(i * MAIN, MAIN), MAIN)
        return remote(tu.at[rows], tr.at[rows], t_s.at[0, i], t_r.at[0, i], up)

    def turned_down(i):
        rows = pl.ds(pl.multiple_of(i * MAIN, MAIN), MAIN)
        return remote(tk.at[rows], td.at[rows], t_s.at[1, i], t_r.at[1, i], down)

    def adjoint_up(i):
        rows = pl.ds(pl.multiple_of(i * MAIN, MAIN), MAIN)

        @pl.when(k > 0)
        def _():
            turned_up(i).wait_recv()

        value = hot[pl.ds(pl.multiple_of(PRIM + i * MAIN, MAIN), MAIN), :].astype(F32) + tr[rows, :]
        ta[rows, :] = value
        result = times_g_turned(value)

        @pl.when(k < SLABS - 1)
        def _():
            tu[rows, :] = result
            turned_up(i).start()

        @pl.when(k == SLABS - 1)
        def _():
            tk[rows, :] = result
            turned_down(i).start()

    def adjoint_down(i):
        rows = pl.ds(pl.multiple_of(i * MAIN, MAIN), MAIN)
        turned_down(i).wait_recv()
        tk[rows, :] = times_g_turned(ta[rows, :] + td[rows, :])

        @pl.when(k > 0)
        def _():
            turned_down(i).start()

    def all_adjoint_down():
        @pl.loop(0, NTURN)
        def _(i):
            adjoint_down(i)

    def setup_z_in():
        arrived(setup_z)
        start(setup_x)

    def setup_x_in():
        arrived(setup_x)
        start(setup_c)

    def setup_core_in():
        arrived(setup_c)
        for half in range(2):
            high, low = split(gs[:, 16 * half : 16 * half + 16, :].reshape(IFACE, 128))
            es[2 * k + half] = dot(hot[0:PRIM, :], high) + dot(hot[0:PRIM, :], low)
        start(ey)

    def coarse_operator():
        arrived(ey)
        for a in range(4):
            ms[a] = jnp.sum(gs[16 * a : 16 * a + 16, 32:40, :], axis=0)
        wide = jnp.concatenate([es[b] for b in range(8)], axis=1)
        both_e = jnp.concatenate(split(wide), axis=0)
        depth = lax.broadcasted_iota(jnp.int32, (IFACE, 256), 0).astype(F32)
        for half in range(2):

            @pl.loop(0, 4)
            def _(t):
                wanted = jnp.concatenate([ms[2 * half, pl.ds(t, 1), :], ms[2 * half + 1, pl.ds(t, 1), :]], axis=1)
                both = dot(both_e, jnp.where(depth == wanted, 1.0, 0.0).astype(BF16))
                high, low = split(both[0:PRIM] + both[PRIM:])
                rows = pl.ds(pl.multiple_of(t * PRIM, PRIM), PRIM)
                ch[rows, 256 * half : 256 * half + 256] = high
                cl[rows, 256 * half : 256 * half + 256] = low

    def give_primal(n, primal):
        tiles = folded([primal[8 * t : 8 * t + 8] for t in range(4)])
        for q in range(4):
            pf[n, q] = tiles[q]
        ps[n, k] = pf[n, k]
        start(fold_y[n])

    def primal_one():
        turned = split(tk[...])
        give_primal(0, three(turned, split(vx[0:RHS, :]), dot_t))

    def solve_sum(n):
        arrived(fold_y[n])
        total = jnp.sum(ps[n], axis=0)
        gp[n, own] = total
        ag[n, k, 0:8, :] = total
        start(coarse_p[n])

    def solve_plane(n):
        arrived(coarse_p[n])
        start(coarse_c[n])

    def solve_core(n):
        arrived(coarse_c[n])
        everyone = split(gp[n].reshape(blocks * 8, 128))
        product = three((ch[...], cl[...]), everyone, dot)
        ag[n, k, 8:16, :] = groups_of(
            [[(product[32 * t + 8 * target : 32 * t + 8 * target + 8], t) for t in range(4)] for target in range(4)]
        )
        start(back_y[n])

    def solved(n):
        arrived(back_y[n])
        tiles = [ag[n, q] for q in range(4)]
        return jnp.concatenate(
            [*folded([tile[0:8] for tile in tiles]), *folded([tile[8:16] for tile in tiles])], axis=0
        )

    def primal_two():
        turned = split(tk[...])
        xys[:, 0:RHS] = three(turned, split(x2[...]), dot_t)
        xys[:, RHS : RHS + EXTRA] = three(turned, split(vx[RHS : RHS + EXTRA, :]), dot_t)

    def solved_one():
        u1 = solved(0)
        u1s[...] = u1
        give_primal(1, xys[:, 0:RHS] - dot3(xys[:, RHS : RHS + EXTRA], u1))

    def base_of_result():
        u1 = u1s[...]
        weights = jnp.concatenate([u1, u1], axis=0).T
        base = jnp.concatenate([-n1[RHS : RHS + EXTRA, :], w0[...]], axis=0)
        out_ref[...] = n1[0:RHS, :] + dot3(weights, base)

    sum0, plane0, core0 = (once(act, 0) for act in (solve_sum, solve_plane, solve_core))
    sum1, plane1, core1 = (once(act, 1) for act in (solve_sum, solve_plane, solve_core))
    setup_z_at, setup_x_at, setup_core_at = map(once, (setup_z_in, setup_x_in, setup_core_in))
    primal_at, solved_at = once(primal_one), once(solved_one)

    def backward_early(i):
        backward_two(*main_chunk(i))

    def backward_late(sem, rows):
        @pl.when((k != 2) | (sem >= EARLY))
        def _():
            backward_two(sem, rows)

    start(setup_z)
    only((1, 2, 3), bases)
    only((2, 3), setup_z_in)

    @pl.loop(0, NTURN)
    def _(i):
        adjoint_up(i)

    only((3,), setup_x_in)
    over_main(
        forward_one,
        [
            (setup_z_at, {0: [5], 1: [0]}),
            (setup_x_at, {1: [6], 2: [3]}),
            (setup_core_at, {2: [4], 3: [0]}),
            (adjoint_down, {2: [5, 6]}),
        ],
    )
    only((0,), bases, all_side_forward, setup_x_in, setup_core_in)
    only((1,), setup_core_in, all_side_forward)
    only((0, 1), coarse_operator, all_adjoint_down)
    only((0, 3), primal_one)
    over_main(
        between,
        [(primal_at, {1: [1], 2: [2]}), (side_forward, {2: [4, 6]}), (sum0, {0: [1], 1: [6]})],
    )
    only((2, 3), coarse_operator)
    only((3,), all_side_forward)
    only((2, 3), sum0)
    only((2,), all_side_backward)
    primal_two()
    only((0, 3), plane0)
    only((0, 3), core0)
    over_main(
        forward_two,
        [
            (backward_early, {2: list(range(NMAIN - EARLY, NMAIN))}),
            (side_backward, {1: [3]}),
            (plane0, {1: [4], 2: [1]}),
            (core0, {1: [5], 2: [2]}),
            (solved_at, {2: [5], 3: [2]}),
            (sum1, {3: [4]}),
        ],
    )
    only((0, 1), solved_one)
    only((1,), lambda: side_backward(1))
    only((0,), all_side_backward)
    only((0, 1), sum1)
    only((0,), base_of_result)
    over_main(
        backward_late,
        [(sum1, {2: [3]}), (plane1, {0: [0], 1: [2], 2: [7]}), (core1, {0: [2], 1: [4]})],
    )
    only((3,), plane1)
    only((1, 2, 3), base_of_result)
    only((2, 3), core1)
    weights = jnp.concatenate([solved(1), jnp.zeros((EXTRA, RHS), F32)], axis=0).T
    out_ref[...] += n2[...] + dot3(weights[:, 0:EXTRA], w0[...])

    for copies in (
        setup_z, setup_x, setup_c, ey, *coarse_p, *coarse_c, *fold_y, *back_y,
    ):
        sent(copies)

    @pl.loop(0, NTURN)
    def _(i):
        @pl.when(k < SLABS - 1)
        def _():
            turned_up(i).wait_send()

        @pl.when(k > 0)
        def _():
            turned_down(i).wait_send()

    def sent_chunk(first):
        def step(sem, rows):
            @pl.when(k < SLABS - 1)
            def _():
                (f1_copy if first else f2_copy)(sem, rows).wait_send()

            @pl.when(k > 0)
            def _():
                (b1_copy if first else b2_copy)(sem, rows).wait_send()

        return step

    over_main(sent_chunk(True))
    over_side(sent_chunk(True))
    over_main(sent_chunk(False))


def on_device(nz, nx, residual, inverse_slab, diagonal, primal_index, coarse_map, schur, basis_one, basis_two, cinv):
    blocks = nz * nx * 2
    dma = pltpu.SemaphoreType.DMA
    vmem = pl.BlockSpec(memory_space=pltpu.VMEM)
    hbm = pl.BlockSpec(memory_space=pl.ANY)
    wide = lambda rows, kind=F32: pltpu.VMEM((rows, IFACE), kind)
    out = pl.pallas_call(
        functools.partial(kernel, nz, nx),
        out_shape=jax.ShapeDtypeStruct((RHS, IFACE), F32),
        in_specs=[hbm] * 9,
        out_specs=vmem,
        scratch_shapes=[
            wide(1),
            *[pltpu.VMEM((1, PRIM), jnp.int32)] * 2,
            pltpu.VMEM((PRIM, PRIM), F32),
            wide(IFACE // blocks),
            wide(IFACE), wide(PRIM), wide(IFACE, BF16), wide(IFACE, BF16),
            *[wide(RHS + EXTRA)] * 5,
            *[wide(RHS)] * 5,
            wide(EXTRA),
            *[wide(PRIM)] * 5,
            wide(EXTRA, BF16),
            pltpu.VMEM((blocks, BLOCK, 128), F32),
            pltpu.VMEM((4, 8, 128), F32),
            pltpu.VMEM((8, PRIM, 128), F32),
            *[pltpu.VMEM((128, blocks * 8), BF16)] * 2,
            *[pltpu.VMEM((2, 4, 8, 128), F32)] * 2,
            pltpu.VMEM((2, blocks, 8, 128), F32),
            pltpu.VMEM((2, 4, 16, 128), F32),
            pltpu.VMEM((EXTRA, RHS), F32),
            pltpu.VMEM((PRIM, RHS + EXTRA), F32),
            dma((PIECES + 8,)),
            *[dma((NMAIN + NSIDE,))] * 4,
            *[dma((NMAIN,))] * 4,
            dma((2, NTURN)), dma((2, NTURN)),
            dma((nx,)), dma((nx,)), dma((nz,)), dma((nz,)), dma((2, nz * nx - 1)), dma((2, nz * nx - 1)), dma((3,)), dma((3,)),
            dma((5, SLABS)), dma((5, SLABS)),
        ],
        compiler_params=pltpu.CompilerParams(
            collective_id=0, has_side_effects=True, vmem_limit_bytes=56 * 2**20
        ),
    )(
        residual[0, 0], inverse_slab[0, 0], basis_one[0, 0], basis_two[0, 0], diagonal[0], primal_index[0],
        coarse_map, schur[0], cinv.T,
    )
    return out[None, None]


def solution(mesh):
    nz, nx = 8, 4
    torus = Mesh(mesh.devices.reshape(nz, nx, 2, mesh.shape["slab"]), (*SUB, "slab"))
    in_specs = (
        P(SUB, "slab", None, None),
        P(SUB, "slab", None, None),
        P(SUB, "slab", None),
        P(SUB, "slab", None),
        P(SUB, None),
        P(SUB, None, None),
        P(SUB, "slab", None, None),
        P(SUB, "slab", None, None),
        P(None, SUB),
    )
    return jax.shard_map(
        functools.partial(on_device, nz, nx),
        mesh=torus,
        in_specs=in_specs,
        out_specs=P(SUB, "slab", None, None),
        check_vma=False,
    )
```

```python
import functools

import jax
import jax.numpy as jnp
from jax import lax
from jax.experimental import pallas as pl
from jax.experimental.pallas import tpu as pltpu
from jax.sharding import Mesh
from jax.sharding import PartitionSpec as P

SUB = ("z", "x", "core")
MESH = pl.DeviceIdType.MESH
F32 = jnp.float32
BF16 = jnp.bfloat16

RHS = 128
IFACE = 1024
PRIM = 32
EXTRA = 2 * PRIM
SLABS = 4
EARLY_Z = 4
LEADER = (5, 2)
MAIN = 16
SIDE = 32
NMAIN = RHS // MAIN
NTURN = PRIM // MAIN
EARLY = 3
NSIDE = EXTRA // SIDE
BLOCK = 40
PIECES = 8


def split(value):
    high = value.astype(BF16)
    return high, (value - high.astype(F32)).astype(BF16)


def dot(left, right):
    return jnp.dot(left, right, preferred_element_type=F32)


def dot_t(left, right):
    return lax.dot_general(left, right, (((1,), (1,)), ((), ())), preferred_element_type=F32)


def three(left, right, times):
    rows = left[0].shape[0]
    both = times(jnp.concatenate(left, axis=0), right[0])
    return both[:rows] + both[rows:] + times(left[0], right[1])


def dot3(left, right):
    return three(split(left), split(right), dot)


def column_of(row):
    eye = lax.broadcasted_iota(jnp.int32, (PRIM, PRIM), 0) == lax.broadcasted_iota(
        jnp.int32, (PRIM, PRIM), 1
    )
    return jnp.sum(jnp.where(eye, jnp.broadcast_to(row, (PRIM, PRIM)), 0.0), axis=1, keepdims=True)


def onehot_of(column, width):
    lanes = lax.broadcasted_iota(jnp.int32, (PRIM, width), 1).astype(F32)
    return jnp.where(lanes == column, 1.0, 0.0).astype(BF16)


def moved(tile, source, target):
    shift = 32 * (target - source) % 128
    return pltpu.roll(tile, shift, 1) if shift else tile


def groups_of(pieces):
    group = lax.broadcasted_iota(jnp.int32, (8, 128), 1) // 32
    total = jnp.zeros((8, 128), F32)
    for target, parts in enumerate(pieces):
        value = sum(moved(tile, source, target) for tile, source in parts)
        total = jnp.where(group == target, value, total)
    return total


def folded(tiles):
    return [groups_of([[(tiles[q], t)] for q in range(4)]) for t in range(4)]


def kernel(
    nz, nx,
    res_hbm, g_hbm, cb_hbm, cbas_hbm, diag_hbm, idx_hbm, map_hbm, schur_hbm, cinv_hbm, out_ref,
    diag_ref, idx_ref, map_ref, schur_ref, cinv_ref, g, cb, ghi, glo, vx, r1, f1, rb1, n1, x2, r2, f2, rb2, n2, w0,
    ta, tu, tr, tk, td, hot, gs, ms, es, eh, ch, cl, pf, ps, gp, ag, u1s, xys,
    in_s, f1_s, f1_r, b1_s, b1_r, f2_s, f2_r, b2_s, b2_r, t_s, t_r,
    gx_s, gx_r, gz_s, gz_r, gp_s, gp_r, gc_s, gc_r, y_s, y_r, ready,
):
    k = lax.axis_index("slab")
    z, x, core = lax.axis_index("z"), lax.axis_index("x"), lax.axis_index("core")
    blocks = 2 * nx * nz

    piece = IFACE // PIECES
    loads = [
        pltpu.make_async_copy(g_hbm.at[pl.ds(i * piece, piece)], g.at[pl.ds(i * piece, piece)], in_s.at[i])
        for i in range(PIECES)
    ]
    small = [
        pltpu.make_async_copy(src, dst, in_s.at[PIECES + 3 + i])
        for i, (src, dst) in enumerate(
            [(map_hbm, map_ref), (idx_hbm, idx_ref), (cinv_hbm, cinv_ref), (diag_hbm, diag_ref), (schur_hbm, schur_ref)]
        )
    ]
    load_res = pltpu.make_async_copy(res_hbm, vx.at[pl.ds(0, RHS)], in_s.at[PIECES])
    load_cb = pltpu.make_async_copy(cb_hbm, cb, in_s.at[PIECES + 1])
    load_cbas = pltpu.make_async_copy(cbas_hbm, w0.at[pl.ds(PRIM, PRIM)], in_s.at[PIECES + 2])
    for copy in (*small[:3], *loads, load_res, *small[3:], load_cb, load_cbas):
        copy.start()

    barrier = pltpu.get_barrier_semaphore()
    plane = [
        {"z": lax.rem(z + dz, nz), "x": lax.rem(x + dx, nx)}
        for dz in sorted(range(nz), key=lambda d: -min(d, nz - d))
        for dx in sorted(range(nx), key=lambda d: -min(d, nx - d))
        if dz or dx
    ]
    leads = (z == LEADER[0]) & (x == LEADER[1])

    def greet(other):
        pl.semaphore_signal(barrier, inc=1, device_id=other, device_id_type=MESH)

    for d in range(1, SLABS):
        greet({"slab": lax.rem(k + d, SLABS)})
    greet({"core": 1 - core})

    @pl.when(jnp.logical_not(leads))
    def _():
        greet({"z": LEADER[0], "x": LEADER[1]})

    own = (core * nx + x) * nz + z

    @pl.when(k == 0)
    def _():
        r1[...] = jnp.zeros_like(r1)
        tr[...] = jnp.zeros_like(tr)

    for copy in small[:3]:
        copy.wait()
    map_row = map_ref[...]
    map_col = column_of(map_row.astype(F32))
    owner, inner = map_row >> 4, map_row & 15
    place = (((owner & 1) * nx + ((owner >> 1) & 3)) * nz + (owner >> 3)) * 16 + inner
    hot[0:PRIM, :] = onehot_of(column_of(place.astype(F32)), IFACE)
    hot[PRIM:EXTRA, :] = onehot_of(column_of(idx_ref[...].astype(F32)), IFACE)

    quarter = pl.ds(pl.multiple_of(k * 256, 256), 256)
    gs[own, 0:16, :] = cinv_ref[:, quarter][:, 0:128]
    gs[own, 16:32, :] = cinv_ref[:, quarter][:, 128:256]
    lanes = lax.broadcasted_iota(jnp.int32, (PRIM, 128), 1)
    subl = lax.broadcasted_iota(jnp.int32, (PRIM, 128), 0)
    spread = jnp.where(lanes - 8 * lax.rem(own, 16) == subl % 8, jnp.broadcast_to(map_col, (PRIM, 128)), 0.0)
    for t in range(4):
        gs[own, 32 + t : 33 + t, :] = jnp.sum(spread[8 * t : 8 * t + 8], axis=0, keepdims=True)
    gs[own, 36:40, :] = jnp.zeros((4, 128), F32)

    def bases():
        for copy in (*small[3:], load_cb, load_cbas):
            copy.wait()
        w0[0:PRIM, :] = -dot3(schur_ref[...], cb[...])
        vx[RHS : RHS + EXTRA, :] = w0[...] * diag_ref[...]

    for i in range(PIECES):
        loads[i].wait()

        @pl.loop(0, piece // 64)
        def _(j):
            rows = pl.ds(pl.multiple_of(i * piece + j * 64, 64), 64)
            high, low = split(g[rows, :])
            ghi[rows, :] = high
            glo[rows, :] = low

    load_res.wait()
    pl.semaphore_wait(barrier, jnp.where(leads, SLABS + len(plane), SLABS))

    @pl.when(leads)
    def _():
        for other in plane:
            pl.semaphore_signal(ready, inc=1, device_id=other, device_id_type=MESH)

    def plane_ready():
        @pl.when(jnp.logical_not(leads))
        def _():
            pl.semaphore_wait(ready, 1)

        start(setup_z)


    def remote(src, dst, send, recv, to):
        return pltpu.make_async_remote_copy(
            src_ref=src, dst_ref=dst, send_sem=send, recv_sem=recv, device_id=to, device_id_type=MESH
        )

    up = {"slab": lax.rem(k + 1, SLABS)}
    down = {"slab": lax.rem(k + SLABS - 1, SLABS)}

    def gather_z(buf):
        return [
            remote(buf.at[own], buf.at[own], gz_s.at[d], gz_r.at[d], {"z": lax.rem(z + d, nz)})
            for d in range(1, nz)
        ]

    def gather_x(buf):
        part = pl.ds((core * nx + x) * nz, nz)
        return [
            remote(buf.at[part], buf.at[part], gx_s.at[d], gx_r.at[d], {"x": lax.rem(x + d, nx)})
            for d in range(1, nx)
        ]

    def gather_plane(buf, n):
        return [
            remote(buf.at[own], buf.at[own], gp_s.at[n, d], gp_r.at[n, d], other) for d, other in enumerate(plane)
        ]

    def gather_core(buf, n):
        part = pl.ds(core * nx * nz, nx * nz)
        return [remote(buf.at[part], buf.at[part], gc_s.at[n], gc_r.at[n], {"core": 1 - core})]

    def to_slabs(copy_of, n):
        made = []
        for d in range(1, SLABS):
            other = lax.rem(k + d, SLABS)
            src, dst = copy_of(other)
            made.append(remote(src, dst, y_s.at[n, d], y_r.at[n, d], {"slab": other}))
        return made

    def start(copies):
        for copy in copies:
            copy.start()

    def arrived(copies):
        for copy in copies:
            copy.wait_recv()

    def sent(copies):
        for copy in copies:
            copy.wait_send()

    setup_z, setup_x, setup_c = gather_z(gs), gather_x(gs), gather_core(gs, 2)
    e_part = pl.ds(2 * k, 2)
    ey = to_slabs(lambda other: (es.at[e_part], es.at[e_part]), 4)
    coarse_p = [gather_plane(gp.at[n], n) for n in range(2)]
    coarse_c = [gather_core(gp.at[n], n) for n in range(2)]
    fold_y = [to_slabs(lambda other: (pf.at[n, other], ps.at[n, k]), 2 * n) for n in range(2)]
    back_y = [to_slabs(lambda other: (ag.at[n, k], ag.at[n, k]), 2 * n + 1) for n in range(2)]

    def times_g(value):
        return three(split(value), (ghi[...], glo[...]), dot)

    def times_g_turned(value):
        return three(split(value), (ghi[...], glo[...]), dot_t)

    def main_chunk(i):
        return i, pl.ds(pl.multiple_of(i * MAIN, MAIN), MAIN)

    def side_chunk(i):
        return NMAIN + i, pl.ds(pl.multiple_of(RHS + i * SIDE, SIDE), SIDE)

    def f1_copy(sem, rows):
        return remote(f1.at[rows], r1.at[rows], f1_s.at[sem], f1_r.at[sem], up)

    def b1_copy(sem, rows):
        return remote(n1.at[rows], rb1.at[rows], b1_s.at[sem], b1_r.at[sem], down)

    def f2_copy(sem, rows):
        return remote(f2.at[rows], r2.at[rows], f2_s.at[sem], f2_r.at[sem], up)

    def b2_copy(sem, rows):
        return remote(n2.at[rows], rb2.at[rows], b2_s.at[sem], b2_r.at[sem], down)

    def forward_one(sem, rows):
        @pl.when(k > 0)
        def _():
            f1_copy(sem, rows).wait_recv()

        value = times_g(vx[rows, :] + r1[rows, :])
        f1[rows, :] = value

        @pl.when(k < SLABS - 1)
        def _():
            f1_copy(sem, rows).start()

        @pl.when(k == SLABS - 1)
        def _():
            n1[rows, :] = value
            b1_copy(sem, rows).start()

    def backward_one(sem, rows):
        @pl.when(k < SLABS - 1)
        def _():
            b1_copy(sem, rows).wait_recv()
            n1[rows, :] = f1[rows, :] + times_g(rb1[rows, :])

            @pl.when(k > 0)
            def _():
                b1_copy(sem, rows).start()

    def between(sem, rows):
        backward_one(sem, rows)
        value = vx[rows, :] - diag_ref[...] * n1[rows, :]
        x2[rows, :] = value

        @pl.when(k == 0)
        def _():
            f2[rows, :] = times_g(value)
            f2_copy(sem, rows).start()

    def forward_two(sem, rows):
        @pl.when(k > 0)
        def _():
            f2_copy(sem, rows).wait_recv()
            value = times_g(x2[rows, :] + r2[rows, :])
            f2[rows, :] = value

            @pl.when(k < SLABS - 1)
            def _():
                f2_copy(sem, rows).start()

            @pl.when(k == SLABS - 1)
            def _():
                n2[rows, :] = value
                b2_copy(sem, rows).start()

    def backward_two(sem, rows):
        @pl.when(k < SLABS - 1)
        def _():
            b2_copy(sem, rows).wait_recv()
            n2[rows, :] = f2[rows, :] + times_g(rb2[rows, :])

            @pl.when(k > 0)
            def _():
                b2_copy(sem, rows).start()

    early = z < EARLY_Z

    def here(who):
        if isinstance(who, int):
            return k == who
        return (k == who[0]) & (early if who[1] else jnp.logical_not(early))

    def over_main(step, hooks=()):
        @pl.loop(0, NMAIN)
        def _(i):
            step(*main_chunk(i))
            for act, places in hooks:
                spots = [(here(who), at) for who, chunks in places.items() for at in chunks]
                due = functools.reduce(jnp.logical_or, [mine & (i == at) for mine, at in spots])
                done = sum(jnp.where(mine & (i > at), 1, 0) for mine, at in spots)

                @pl.when(due)
                def _():
                    act(done)

    def over_side(step):
        @pl.loop(0, NSIDE)
        def _(i):
            step(*side_chunk(i))

    def only(those, *acts):
        @pl.when(functools.reduce(jnp.logical_or, [here(who) for who in those]))
        def _():
            for act in acts:
                act()

    def once(act, *args):
        return lambda *_: act(*args)

    def side_forward(i):
        forward_one(*side_chunk(i))

    def side_backward(i):
        backward_one(*side_chunk(i))

    def all_side_forward():
        over_side(forward_one)

    def all_side_backward():
        over_side(backward_one)

    def turned_up(i):
        rows = pl.ds(pl.multiple_of(i * MAIN, MAIN), MAIN)
        return remote(tu.at[rows], tr.at[rows], t_s.at[0, i], t_r.at[0, i], up)

    def turned_down(i):
        rows = pl.ds(pl.multiple_of(i * MAIN, MAIN), MAIN)
        return remote(tk.at[rows], td.at[rows], t_s.at[1, i], t_r.at[1, i], down)

    def adjoint_up(i):
        rows = pl.ds(pl.multiple_of(i * MAIN, MAIN), MAIN)

        @pl.when(k > 0)
        def _():
            turned_up(i).wait_recv()

        value = hot[pl.ds(pl.multiple_of(PRIM + i * MAIN, MAIN), MAIN), :].astype(F32) + tr[rows, :]
        ta[rows, :] = value
        result = times_g_turned(value)

        @pl.when(k < SLABS - 1)
        def _():
            tu[rows, :] = result
            turned_up(i).start()

        @pl.when(k == SLABS - 1)
        def _():
            tk[rows, :] = result
            turned_down(i).start()

    def adjoint_down(i):
        rows = pl.ds(pl.multiple_of(i * MAIN, MAIN), MAIN)
        turned_down(i).wait_recv()
        tk[rows, :] = times_g_turned(ta[rows, :] + td[rows, :])

        @pl.when(k > 0)
        def _():
            turned_down(i).start()

    def all_adjoint_down():
        @pl.loop(0, NTURN)
        def _(i):
            adjoint_down(i)

    def setup_z_in():
        arrived(setup_z)
        start(setup_x)

    def setup_x_in():
        arrived(setup_x)
        start(setup_c)

    def setup_core_in():
        arrived(setup_c)
        for half in range(2):
            high, low = split(gs[:, 16 * half : 16 * half + 16, :].reshape(IFACE, 128))
            es[2 * k + half] = dot(hot[0:PRIM, :], high) + dot(hot[0:PRIM, :], low)
        start(ey)

    def operator_base():
        arrived(ey)
        for a in range(4):
            ms[a] = jnp.sum(gs[16 * a : 16 * a + 16, 32:40, :], axis=0)
        wide = jnp.concatenate([es[b] for b in range(8)], axis=1)
        eh[...] = jnp.concatenate(split(wide), axis=0)

    def operator_piece(i):
        t, half = i // 2, i % 2
        depth = lax.broadcasted_iota(jnp.int32, (IFACE, 256), 0).astype(F32)
        wanted = jnp.concatenate([ms[2 * half, pl.ds(t, 1), :], ms[2 * half + 1, pl.ds(t, 1), :]], axis=1)
        both = dot(eh[...], jnp.where(depth == wanted, 1.0, 0.0).astype(BF16))
        high, low = split(both[0:PRIM] + both[PRIM:])
        rows, columns = pl.ds(pl.multiple_of(t * PRIM, PRIM), PRIM), pl.ds(pl.multiple_of(half * 256, 256), 256)
        ch[rows, columns] = high
        cl[rows, columns] = low

    def coarse_operator():
        operator_base()

        @pl.loop(0, 8)
        def _(i):
            operator_piece(i)

    def give_primal(n, primal):
        tiles = folded([primal[8 * t : 8 * t + 8] for t in range(4)])
        for q in range(4):
            pf[n, q] = tiles[q]
        ps[n, k] = pf[n, k]
        start(fold_y[n])

    def primal_one():
        turned = split(tk[...])
        give_primal(0, three(turned, split(vx[0:RHS, :]), dot_t))

    def solve_sum(n):
        arrived(fold_y[n])
        total = jnp.sum(ps[n], axis=0)
        gp[n, own] = total
        ag[n, k, 0:8, :] = total
        start(coarse_p[n])

    def solve_plane(n):
        arrived(coarse_p[n])
        start(coarse_c[n])

    def solve_core(n):
        arrived(coarse_c[n])
        everyone = split(gp[n].reshape(blocks * 8, 128))
        product = three((ch[...], cl[...]), everyone, dot)
        ag[n, k, 8:16, :] = groups_of(
            [[(product[32 * t + 8 * target : 32 * t + 8 * target + 8], t) for t in range(4)] for target in range(4)]
        )
        start(back_y[n])

    def solved(n):
        arrived(back_y[n])
        tiles = [ag[n, q] for q in range(4)]
        return jnp.concatenate(
            [*folded([tile[0:8] for tile in tiles]), *folded([tile[8:16] for tile in tiles])], axis=0
        )

    def primal_two():
        turned = split(tk[...])
        xys[:, 0:RHS] = three(turned, split(x2[...]), dot_t)
        xys[:, RHS : RHS + EXTRA] = three(turned, split(vx[RHS : RHS + EXTRA, :]), dot_t)

    def solved_one():
        u1 = solved(0)
        u1s[...] = u1
        give_primal(1, xys[:, 0:RHS] - dot3(xys[:, RHS : RHS + EXTRA], u1))

    def base_of_result():
        u1 = u1s[...]
        weights = jnp.concatenate([u1, u1], axis=0).T
        base = jnp.concatenate([-n1[RHS : RHS + EXTRA, :], w0[...]], axis=0)
        out_ref[...] = n1[0:RHS, :] + dot3(weights, base)

    sum0, plane0, core0 = (once(act, 0) for act in (solve_sum, solve_plane, solve_core))
    sum1, plane1, core1 = (once(act, 1) for act in (solve_sum, solve_plane, solve_core))
    setup_z_at, setup_x_at, setup_core_at = map(once, (setup_z_in, setup_x_in, setup_core_in))
    primal_at, solved_at, ready_at = once(primal_one), once(solved_one), once(plane_ready)

    def side_backward_last():
        side_backward(NSIDE - 1)

    def operator_piece_late(i):
        operator_piece(3 + i)

    def backward_early(i):
        backward_two(*main_chunk(i))

    def backward_late(sem, rows):
        @pl.when((k != 2) | (sem >= EARLY))
        def _():
            backward_two(sem, rows)

    only((1, 2, 3), bases)
    only(((1, 0), 2, 3), plane_ready)
    only(((2, 0), (3, 0)), setup_z_in)

    @pl.loop(0, NTURN)
    def _(i):
        adjoint_up(i)

    only(((3, 1),), setup_z_in)
    over_main(
        forward_one,
        [
            (ready_at, {(0, 0): [1], (1, 1): [1]}),
            (setup_z_at, {(1, 0): [4], (1, 1): [5], (2, 1): [3]}),
            (setup_x_at, {(2, 0): [4], (3, 0): [0], (3, 1): [6]}),
            (setup_core_at, {(2, 0): [6], (3, 0): [2], (3, 1): [7]}),
            (adjoint_down, {2: [5, 6]}),
        ],
    )
    only(((0, 1),), plane_ready)
    only((0,), bases, all_side_forward, setup_z_in, setup_x_in, setup_core_in)
    only((1,), all_side_forward, setup_x_in)
    only((0, 1), all_adjoint_down)
    only((0, 3), primal_one)
    over_main(
        between,
        [
            (primal_at, {1: [1], 2: [2]}),
            (setup_x_at, {(2, 1): [1]}),
            (setup_core_at, {1: [0], (2, 1): [3]}),
            (once(operator_base), {1: [5]}),
            (operator_piece, {1: [5, 6, 7]}),
            (side_forward, {2: [4, 6]}),
            (sum0, {0: [1], 1: [6]}),
        ],
    )
    only((0,), coarse_operator)
    only((3,), all_side_forward)
    only((2, 3), sum0, coarse_operator)
    only((2,), all_side_backward)
    primal_two()
    only((0, (3, 0)), plane0, core0)
    over_main(
        forward_two,
        [
            (backward_early, {2: list(range(NMAIN - EARLY, NMAIN))}),
            (operator_piece_late, {1: list(range(5))}),
            (side_backward, {1: [3]}),
            (plane0, {(1, 0): [4], (1, 1): [6], (2, 0): [1], (2, 1): [3], (3, 1): [0]}),
            (core0, {(1, 0): [5], (1, 1): [7], (2, 0): [2], (2, 1): [4], (3, 1): [1]}),
            (solved_at, {(2, 0): [6], (2, 1): [7], 3: [3]}),
            (sum1, {(3, 0): [5], (3, 1): [6]}),
        ],
    )
    only(((1, 1),), side_backward_last)
    only((0, 1), solved_one)
    only(((1, 0),), side_backward_last)
    only((0,), all_side_backward)
    only((0, (1, 0)), sum1)
    only((0,), base_of_result)
    over_main(
        backward_late,
        [
            (sum1, {(1, 1): [0], (2, 0): [3], (2, 1): [4]}),
            (plane1, {(0, 0): [2], (0, 1): [4], (1, 0): [5], (1, 1): [6], (2, 0): [7]}),
            (core1, {(0, 0): [4], (0, 1): [5], (1, 0): [7]}),
        ],
    )
    only(((2, 1), 3), plane1)
    only((1, 2, 3), base_of_result)
    only(((1, 1), 2, 3), core1)
    weights = jnp.concatenate([solved(1), jnp.zeros((EXTRA, RHS), F32)], axis=0).T
    out_ref[...] += n2[...] + dot3(weights[:, 0:EXTRA], w0[...])

    for copies in (
        setup_z, setup_x, setup_c, ey, *coarse_p, *coarse_c, *fold_y, *back_y,
    ):
        sent(copies)

    @pl.loop(0, NTURN)
    def _(i):
        @pl.when(k < SLABS - 1)
        def _():
            turned_up(i).wait_send()

        @pl.when(k > 0)
        def _():
            turned_down(i).wait_send()

    def sent_chunk(first):
        def step(sem, rows):
            @pl.when(k < SLABS - 1)
            def _():
                (f1_copy if first else f2_copy)(sem, rows).wait_send()

            @pl.when(k > 0)
            def _():
                (b1_copy if first else b2_copy)(sem, rows).wait_send()

        return step

    over_main(sent_chunk(True))
    over_side(sent_chunk(True))
    over_main(sent_chunk(False))


def on_device(nz, nx, residual, inverse_slab, diagonal, primal_index, coarse_map, schur, basis_one, basis_two, cinv):
    blocks = nz * nx * 2
    dma = pltpu.SemaphoreType.DMA
    vmem = pl.BlockSpec(memory_space=pltpu.VMEM)
    hbm = pl.BlockSpec(memory_space=pl.ANY)
    wide = lambda rows, kind=F32: pltpu.VMEM((rows, IFACE), kind)
    out = pl.pallas_call(
        functools.partial(kernel, nz, nx),
        out_shape=jax.ShapeDtypeStruct((RHS, IFACE), F32),
        in_specs=[hbm] * 9,
        out_specs=vmem,
        scratch_shapes=[
            wide(1),
            *[pltpu.VMEM((1, PRIM), jnp.int32)] * 2,
            pltpu.VMEM((PRIM, PRIM), F32),
            wide(IFACE // blocks),
            wide(IFACE), wide(PRIM), wide(IFACE, BF16), wide(IFACE, BF16),
            *[wide(RHS + EXTRA)] * 5,
            *[wide(RHS)] * 5,
            wide(EXTRA),
            *[wide(PRIM)] * 5,
            wide(EXTRA, BF16),
            pltpu.VMEM((blocks, BLOCK, 128), F32),
            pltpu.VMEM((4, 8, 128), F32),
            pltpu.VMEM((8, PRIM, 128), F32),
            wide(EXTRA, BF16),
            *[pltpu.VMEM((128, blocks * 8), BF16)] * 2,
            *[pltpu.VMEM((2, 4, 8, 128), F32)] * 2,
            pltpu.VMEM((2, blocks, 8, 128), F32),
            pltpu.VMEM((2, 4, 16, 128), F32),
            pltpu.VMEM((EXTRA, RHS), F32),
            pltpu.VMEM((PRIM, RHS + EXTRA), F32),
            dma((PIECES + 8,)),
            *[dma((NMAIN + NSIDE,))] * 4,
            *[dma((NMAIN,))] * 4,
            dma((2, NTURN)), dma((2, NTURN)),
            dma((nx,)), dma((nx,)), dma((nz,)), dma((nz,)), dma((2, nz * nx - 1)), dma((2, nz * nx - 1)), dma((3,)), dma((3,)),
            dma((5, SLABS)), dma((5, SLABS)), pltpu.SemaphoreType.REGULAR,
        ],
        compiler_params=pltpu.CompilerParams(
            collective_id=0, has_side_effects=True, vmem_limit_bytes=56 * 2**20
        ),
    )(
        residual[0, 0], inverse_slab[0, 0], basis_one[0, 0], basis_two[0, 0], diagonal[0], primal_index[0],
        coarse_map, schur[0], cinv.T,
    )
    return out[None, None]


def solution(mesh):
    nz, nx = 8, 4
    torus = Mesh(mesh.devices.reshape(nz, nx, 2, mesh.shape["slab"]), (*SUB, "slab"))
    in_specs = (
        P(SUB, "slab", None, None),
        P(SUB, "slab", None, None),
        P(SUB, "slab", None),
        P(SUB, "slab", None),
        P(SUB, None),
        P(SUB, None, None),
        P(SUB, "slab", None, None),
        P(SUB, "slab", None, None),
        P(None, SUB),
    )
    return jax.shard_map(
        functools.partial(on_device, nz, nx),
        mesh=torus,
        in_specs=in_specs,
        out_specs=P(SUB, "slab", None, None),
        check_vma=False,
    )
```

```python
import functools

import jax
import jax.numpy as jnp
from jax import lax
from jax.experimental import pallas as pl
from jax.experimental.pallas import tpu as pltpu
from jax.sharding import Mesh
from jax.sharding import PartitionSpec as P

SUB = ("z", "x", "core")
MESH = pl.DeviceIdType.MESH
F32 = jnp.float32
BF16 = jnp.bfloat16

RHS = 128
IFACE = 1024
PRIM = 32
EXTRA = 2 * PRIM
SLABS = 4
EARLY_Z = 3
LEADER = (5, 2)
MAIN = 16
SIDE = 32
NMAIN = RHS // MAIN
NTURN = PRIM // MAIN
EARLY = 3
NSIDE = EXTRA // SIDE
BLOCK = 40
PIECES = 8


def split(value):
    high = value.astype(BF16)
    return high, (value - high.astype(F32)).astype(BF16)


def dot(left, right):
    return jnp.dot(left, right, preferred_element_type=F32)


def dot_t(left, right):
    return lax.dot_general(left, right, (((1,), (1,)), ((), ())), preferred_element_type=F32)


def three(left, right, times):
    rows = left[0].shape[0]
    both = times(jnp.concatenate(left, axis=0), right[0])
    return both[:rows] + both[rows:] + times(left[0], right[1])


def dot3(left, right):
    return three(split(left), split(right), dot)


def column_of(row):
    eye = lax.broadcasted_iota(jnp.int32, (PRIM, PRIM), 0) == lax.broadcasted_iota(
        jnp.int32, (PRIM, PRIM), 1
    )
    return jnp.sum(jnp.where(eye, jnp.broadcast_to(row, (PRIM, PRIM)), 0.0), axis=1, keepdims=True)


def onehot_of(column, width):
    lanes = lax.broadcasted_iota(jnp.int32, (PRIM, width), 1).astype(F32)
    return jnp.where(lanes == column, 1.0, 0.0).astype(BF16)


def moved(tile, source, target):
    shift = 32 * (target - source) % 128
    return pltpu.roll(tile, shift, 1) if shift else tile


def groups_of(pieces):
    group = lax.broadcasted_iota(jnp.int32, (8, 128), 1) // 32
    total = jnp.zeros((8, 128), F32)
    for target, parts in enumerate(pieces):
        value = sum(moved(tile, source, target) for tile, source in parts)
        total = jnp.where(group == target, value, total)
    return total


def folded(tiles):
    return [groups_of([[(tiles[q], t)] for q in range(4)]) for t in range(4)]


def kernel(
    nz, nx,
    res_hbm, g_hbm, cb_hbm, cbas_hbm, diag_hbm, idx_hbm, map_hbm, schur_hbm, cinv_hbm, out_hbm,
    out_ref, diag_ref, idx_ref, map_ref, schur_ref, cinv_ref, g, cb, ghi, glo, vx, r1, f1, rb1, n1, x2, r2, f2, rb2, n2, w0,
    ta, tu, tr, tk, td, hot, gs, ms, es, eh, ch, cl, pf, ps, gp, ag, u1s, xys,
    in_s, out_s, f1_s, f1_r, b1_s, b1_r, f2_s, f2_r, b2_s, b2_r, t_s, t_r,
    gx_s, gx_r, gz_s, gz_r, gp_s, gp_r, gc_s, gc_r, y_s, y_r, ready,
):
    k = lax.axis_index("slab")
    z, x, core = lax.axis_index("z"), lax.axis_index("x"), lax.axis_index("core")
    blocks = 2 * nx * nz

    piece = IFACE // PIECES
    loads = [
        pltpu.make_async_copy(g_hbm.at[pl.ds(i * piece, piece)], g.at[pl.ds(i * piece, piece)], in_s.at[i])
        for i in range(PIECES)
    ]
    small = [
        pltpu.make_async_copy(src, dst, in_s.at[PIECES + 3 + i])
        for i, (src, dst) in enumerate(
            [(map_hbm, map_ref), (idx_hbm, idx_ref), (cinv_hbm, cinv_ref), (diag_hbm, diag_ref), (schur_hbm, schur_ref)]
        )
    ]
    load_res = pltpu.make_async_copy(res_hbm, vx.at[pl.ds(0, RHS)], in_s.at[PIECES])
    load_cb = pltpu.make_async_copy(cb_hbm, cb, in_s.at[PIECES + 1])
    load_cbas = pltpu.make_async_copy(cbas_hbm, w0.at[pl.ds(PRIM, PRIM)], in_s.at[PIECES + 2])
    for copy in (*small[:3], *loads, load_res, *small[3:], load_cb, load_cbas):
        copy.start()

    barrier = pltpu.get_barrier_semaphore()
    plane = [
        {"z": lax.rem(z + dz, nz), "x": lax.rem(x + dx, nx)}
        for dz in sorted(range(nz), key=lambda d: -min(d, nz - d))
        for dx in sorted(range(nx), key=lambda d: -min(d, nx - d))
        if dz or dx
    ]
    leads = (z == LEADER[0]) & (x == LEADER[1])

    def greet(other):
        pl.semaphore_signal(barrier, inc=1, device_id=other, device_id_type=MESH)

    for d in range(1, SLABS):
        greet({"slab": lax.rem(k + d, SLABS)})
    greet({"core": 1 - core})

    @pl.when(jnp.logical_not(leads))
    def _():
        greet({"z": LEADER[0], "x": LEADER[1]})

    own = (core * nx + x) * nz + z

    @pl.when(k == 0)
    def _():
        r1[...] = jnp.zeros_like(r1)
        tr[...] = jnp.zeros_like(tr)

    for copy in small[:3]:
        copy.wait()
    map_row = map_ref[...]
    map_col = column_of(map_row.astype(F32))
    owner, inner = map_row >> 4, map_row & 15
    place = (((owner & 1) * nx + ((owner >> 1) & 3)) * nz + (owner >> 3)) * 16 + inner
    hot[0:PRIM, :] = onehot_of(column_of(place.astype(F32)), IFACE)
    hot[PRIM:EXTRA, :] = onehot_of(column_of(idx_ref[...].astype(F32)), IFACE)

    quarter = pl.ds(pl.multiple_of(k * 256, 256), 256)
    gs[own, 0:16, :] = cinv_ref[:, quarter][:, 0:128]
    gs[own, 16:32, :] = cinv_ref[:, quarter][:, 128:256]
    lanes = lax.broadcasted_iota(jnp.int32, (PRIM, 128), 1)
    subl = lax.broadcasted_iota(jnp.int32, (PRIM, 128), 0)
    spread = jnp.where(lanes - 8 * lax.rem(own, 16) == subl % 8, jnp.broadcast_to(map_col, (PRIM, 128)), 0.0)
    for t in range(4):
        gs[own, 32 + t : 33 + t, :] = jnp.sum(spread[8 * t : 8 * t + 8], axis=0, keepdims=True)
    gs[own, 36:40, :] = jnp.zeros((4, 128), F32)

    def bases():
        for copy in (*small[3:], load_cb, load_cbas):
            copy.wait()
        w0[0:PRIM, :] = -dot3(schur_ref[...], cb[...])
        vx[RHS : RHS + EXTRA, :] = w0[...] * diag_ref[...]

    for i in range(PIECES):
        loads[i].wait()

        @pl.loop(0, piece // 64)
        def _(j):
            rows = pl.ds(pl.multiple_of(i * piece + j * 64, 64), 64)
            high, low = split(g[rows, :])
            ghi[rows, :] = high
            glo[rows, :] = low

    load_res.wait()
    pl.semaphore_wait(barrier, jnp.where(leads, SLABS + len(plane), SLABS))

    @pl.when(leads)
    def _():
        for other in plane:
            pl.semaphore_signal(ready, inc=1, device_id=other, device_id_type=MESH)

    def plane_ready():
        @pl.when(jnp.logical_not(leads))
        def _():
            pl.semaphore_wait(ready, 1)

        start(setup_z)


    def remote(src, dst, send, recv, to):
        return pltpu.make_async_remote_copy(
            src_ref=src, dst_ref=dst, send_sem=send, recv_sem=recv, device_id=to, device_id_type=MESH
        )

    up = {"slab": lax.rem(k + 1, SLABS)}
    down = {"slab": lax.rem(k + SLABS - 1, SLABS)}

    def gather_z(buf):
        return [
            remote(buf.at[own], buf.at[own], gz_s.at[d], gz_r.at[d], {"z": lax.rem(z + d, nz)})
            for d in range(1, nz)
        ]

    def gather_x(buf):
        part = pl.ds((core * nx + x) * nz, nz)
        return [
            remote(buf.at[part], buf.at[part], gx_s.at[d], gx_r.at[d], {"x": lax.rem(x + d, nx)})
            for d in range(1, nx)
        ]

    def gather_plane(buf, n):
        return [
            remote(buf.at[own], buf.at[own], gp_s.at[n, d], gp_r.at[n, d], other) for d, other in enumerate(plane)
        ]

    def gather_core(buf, n):
        part = pl.ds(core * nx * nz, nx * nz)
        return [remote(buf.at[part], buf.at[part], gc_s.at[n], gc_r.at[n], {"core": 1 - core})]

    def to_slabs(copy_of, n):
        made = []
        for d in range(1, SLABS):
            other = lax.rem(k + d, SLABS)
            src, dst = copy_of(other)
            made.append(remote(src, dst, y_s.at[n, d], y_r.at[n, d], {"slab": other}))
        return made

    def start(copies):
        for copy in copies:
            copy.start()

    def arrived(copies):
        for copy in copies:
            copy.wait_recv()

    def sent(copies):
        for copy in copies:
            copy.wait_send()

    setup_z, setup_x, setup_c = gather_z(gs), gather_x(gs), gather_core(gs, 2)
    e_part = pl.ds(2 * k, 2)
    ey = to_slabs(lambda other: (es.at[e_part], es.at[e_part]), 4)
    coarse_p = [gather_plane(gp.at[n], n) for n in range(2)]
    coarse_c = [gather_core(gp.at[n], n) for n in range(2)]
    fold_y = [to_slabs(lambda other: (pf.at[n, other], ps.at[n, k]), 2 * n) for n in range(2)]
    back_y = [to_slabs(lambda other: (ag.at[n, k], ag.at[n, k]), 2 * n + 1) for n in range(2)]

    def times_g(value):
        return three(split(value), (ghi[...], glo[...]), dot)

    def times_g_turned(value):
        return three(split(value), (ghi[...], glo[...]), dot_t)

    def main_chunk(i):
        return i, pl.ds(pl.multiple_of(i * MAIN, MAIN), MAIN)

    def side_chunk(i):
        return NMAIN + i, pl.ds(pl.multiple_of(RHS + i * SIDE, SIDE), SIDE)

    def f1_copy(sem, rows):
        return remote(f1.at[rows], r1.at[rows], f1_s.at[sem], f1_r.at[sem], up)

    def b1_copy(sem, rows):
        return remote(n1.at[rows], rb1.at[rows], b1_s.at[sem], b1_r.at[sem], down)

    def f2_copy(sem, rows):
        return remote(f2.at[rows], r2.at[rows], f2_s.at[sem], f2_r.at[sem], up)

    def b2_copy(sem, rows):
        return remote(n2.at[rows], rb2.at[rows], b2_s.at[sem], b2_r.at[sem], down)

    def forward_one(sem, rows):
        @pl.when(k > 0)
        def _():
            f1_copy(sem, rows).wait_recv()

        value = times_g(vx[rows, :] + r1[rows, :])
        f1[rows, :] = value

        @pl.when(k < SLABS - 1)
        def _():
            f1_copy(sem, rows).start()

        @pl.when(k == SLABS - 1)
        def _():
            n1[rows, :] = value
            b1_copy(sem, rows).start()

    def backward_one(sem, rows):
        @pl.when(k < SLABS - 1)
        def _():
            b1_copy(sem, rows).wait_recv()
            n1[rows, :] = f1[rows, :] + times_g(rb1[rows, :])

            @pl.when(k > 0)
            def _():
                b1_copy(sem, rows).start()

    def between(sem, rows):
        backward_one(sem, rows)
        value = vx[rows, :] - diag_ref[...] * n1[rows, :]
        x2[rows, :] = value

        @pl.when(k == 0)
        def _():
            f2[rows, :] = times_g(value)
            f2_copy(sem, rows).start()

    def forward_two(sem, rows):
        @pl.when(k > 0)
        def _():
            f2_copy(sem, rows).wait_recv()
            value = times_g(x2[rows, :] + r2[rows, :])
            f2[rows, :] = value

            @pl.when(k < SLABS - 1)
            def _():
                f2_copy(sem, rows).start()

            @pl.when(k == SLABS - 1)
            def _():
                n2[rows, :] = value
                b2_copy(sem, rows).start()

    def backward_two(sem, rows):
        @pl.when(k < SLABS - 1)
        def _():
            b2_copy(sem, rows).wait_recv()
            n2[rows, :] = f2[rows, :] + times_g(rb2[rows, :])

            @pl.when(k > 0)
            def _():
                b2_copy(sem, rows).start()

    early = z < EARLY_Z

    def here(who):
        if isinstance(who, int):
            return k == who
        return (k == who[0]) & (early if who[1] else jnp.logical_not(early))

    def over_main(step, hooks=()):
        @pl.loop(0, NMAIN)
        def _(i):
            step(*main_chunk(i))
            for act, places in hooks:
                spots = [(here(who), at) for who, chunks in places.items() for at in chunks]
                due = functools.reduce(jnp.logical_or, [mine & (i == at) for mine, at in spots])
                done = sum(jnp.where(mine & (i > at), 1, 0) for mine, at in spots)

                @pl.when(due)
                def _():
                    act(done)

    def over_side(step):
        @pl.loop(0, NSIDE)
        def _(i):
            step(*side_chunk(i))

    def only(those, *acts):
        @pl.when(functools.reduce(jnp.logical_or, [here(who) for who in those]))
        def _():
            for act in acts:
                act()

    def once(act, *args):
        return lambda *_: act(*args)

    def side_forward(i):
        forward_one(*side_chunk(i))

    def side_backward(i):
        backward_one(*side_chunk(i))

    def all_side_forward():
        over_side(forward_one)

    def all_side_backward():
        over_side(backward_one)

    def turned_up(i):
        rows = pl.ds(pl.multiple_of(i * MAIN, MAIN), MAIN)
        return remote(tu.at[rows], tr.at[rows], t_s.at[0, i], t_r.at[0, i], up)

    def turned_down(i):
        rows = pl.ds(pl.multiple_of(i * MAIN, MAIN), MAIN)
        return remote(tk.at[rows], td.at[rows], t_s.at[1, i], t_r.at[1, i], down)

    def adjoint_up(i):
        rows = pl.ds(pl.multiple_of(i * MAIN, MAIN), MAIN)

        @pl.when(k > 0)
        def _():
            turned_up(i).wait_recv()

        value = hot[pl.ds(pl.multiple_of(PRIM + i * MAIN, MAIN), MAIN), :].astype(F32) + tr[rows, :]
        ta[rows, :] = value
        result = times_g_turned(value)

        @pl.when(k < SLABS - 1)
        def _():
            tu[rows, :] = result
            turned_up(i).start()

        @pl.when(k == SLABS - 1)
        def _():
            tk[rows, :] = result
            turned_down(i).start()

    def adjoint_down(i):
        rows = pl.ds(pl.multiple_of(i * MAIN, MAIN), MAIN)
        turned_down(i).wait_recv()
        tk[rows, :] = times_g_turned(ta[rows, :] + td[rows, :])

        @pl.when(k > 0)
        def _():
            turned_down(i).start()

    def setup_z_in():
        arrived(setup_z)
        start(setup_x)

    def setup_x_in():
        arrived(setup_x)
        start(setup_c)

    def setup_core_in():
        arrived(setup_c)
        for half in range(2):
            high, low = split(gs[:, 16 * half : 16 * half + 16, :].reshape(IFACE, 128))
            es[2 * k + half] = dot(hot[0:PRIM, :], high) + dot(hot[0:PRIM, :], low)
        start(ey)

    def operator_base():
        arrived(ey)
        for a in range(4):
            ms[a] = jnp.sum(gs[16 * a : 16 * a + 16, 32:40, :], axis=0)
        wide = jnp.concatenate([es[b] for b in range(8)], axis=1)
        eh[...] = jnp.concatenate(split(wide), axis=0)

    def operator_piece(i):
        t, half = i // 2, i % 2
        depth = lax.broadcasted_iota(jnp.int32, (IFACE, 256), 0).astype(F32)
        wanted = jnp.concatenate([ms[2 * half, pl.ds(t, 1), :], ms[2 * half + 1, pl.ds(t, 1), :]], axis=1)
        both = dot(eh[...], jnp.where(depth == wanted, 1.0, 0.0).astype(BF16))
        high, low = split(both[0:PRIM] + both[PRIM:])
        rows, columns = pl.ds(pl.multiple_of(t * PRIM, PRIM), PRIM), pl.ds(pl.multiple_of(half * 256, 256), 256)
        ch[rows, columns] = high
        cl[rows, columns] = low

    def coarse_operator():
        operator_base()

        @pl.loop(0, 8)
        def _(i):
            operator_piece(i)

    def give_primal(n, primal):
        tiles = folded([primal[8 * t : 8 * t + 8] for t in range(4)])
        for q in range(4):
            pf[n, q] = tiles[q]
        ps[n, k] = pf[n, k]
        start(fold_y[n])

    def primal_one():
        turned = split(tk[...])
        give_primal(0, three(turned, split(vx[0:RHS, :]), dot_t))

    def solve_sum(n):
        arrived(fold_y[n])
        total = jnp.sum(ps[n], axis=0)
        gp[n, own] = total
        ag[n, k, 0:8, :] = total
        start(coarse_p[n])

    def solve_plane(n):
        arrived(coarse_p[n])
        start(coarse_c[n])

    def solve_core(n):
        arrived(coarse_c[n])
        everyone = split(gp[n].reshape(blocks * 8, 128))
        product = three((ch[...], cl[...]), everyone, dot)
        ag[n, k, 8:16, :] = groups_of(
            [[(product[32 * t + 8 * target : 32 * t + 8 * target + 8], t) for t in range(4)] for target in range(4)]
        )
        start(back_y[n])

    def solved(n):
        arrived(back_y[n])
        tiles = [ag[n, q] for q in range(4)]
        return jnp.concatenate(
            [*folded([tile[0:8] for tile in tiles]), *folded([tile[8:16] for tile in tiles])], axis=0
        )

    def primal_two():
        turned = split(tk[...])
        xys[:, 0:RHS] = three(turned, split(x2[...]), dot_t)
        xys[:, RHS : RHS + EXTRA] = three(turned, split(vx[RHS : RHS + EXTRA, :]), dot_t)

    def solved_one():
        u1 = solved(0)
        u1s[...] = u1
        give_primal(1, xys[:, 0:RHS] - dot3(xys[:, RHS : RHS + EXTRA], u1))

    def base_of_result():
        u1 = u1s[...]
        weights = jnp.concatenate([u1, u1], axis=0).T
        base = jnp.concatenate([-n1[RHS : RHS + EXTRA, :], w0[...]], axis=0)
        out_ref[...] = n1[0:RHS, :] + dot3(weights, base)

    sum0, plane0, core0 = (once(act, 0) for act in (solve_sum, solve_plane, solve_core))
    sum1, plane1, core1 = (once(act, 1) for act in (solve_sum, solve_plane, solve_core))
    setup_z_at, setup_x_at, setup_core_at = map(once, (setup_z_in, setup_x_in, setup_core_in))
    primal_at, solved_at, ready_at = once(primal_one), once(solved_one), once(plane_ready)

    def side_backward_last():
        side_backward(NSIDE - 1)

    def operator_piece_late(i):
        operator_piece(3 + i)

    def backward_early(i):
        backward_two(*main_chunk(i))

    def backward_late(sem, rows):
        @pl.when((k != 2) | (sem >= EARLY))
        def _():
            backward_two(sem, rows)

    only((1, 2, 3), bases)
    only(((1, 0), 2, 3), plane_ready)
    only(((2, 0), (3, 0)), setup_z_in)

    @pl.loop(0, NTURN)
    def _(i):
        adjoint_up(i)

    only(((3, 1),), setup_z_in)
    over_main(
        forward_one,
        [
            (ready_at, {(0, 0): [1], (1, 1): [1]}),
            (setup_z_at, {(1, 0): [4], (1, 1): [5], (2, 1): [3]}),
            (setup_x_at, {(2, 0): [4], (3, 0): [0], (3, 1): [6]}),
            (setup_core_at, {(2, 0): [6], (3, 0): [2], (3, 1): [7]}),
            (adjoint_down, {2: [5, 6]}),
        ],
    )
    only(((0, 1),), plane_ready)
    only((0,), bases, all_side_forward, setup_z_in, setup_x_in, setup_core_in)
    only((1,), all_side_forward, setup_x_in)
    @pl.when(k < 2)
    def _():
        @pl.loop(0, NTURN)
        def _(i):
            adjoint_down(i)
            pl.when(here((1, 0)) & (i == 0))(setup_core_in)

    only((0, 3), primal_one)
    over_main(
        between,
        [
            (primal_at, {1: [1], 2: [2]}),
            (setup_x_at, {(2, 1): [1]}),
            (setup_core_at, {(1, 1): [0], (2, 1): [3]}),
            (once(operator_base), {1: [5]}),
            (operator_piece, {1: [5, 6, 7]}),
            (side_forward, {2: [4, 6]}),
            (sum0, {0: [1], 1: [6]}),
            (plane0, {(0, 0): [6]}),
        ],
    )
    only((0,), coarse_operator)
    only((3,), all_side_forward)
    only((2, 3), sum0, coarse_operator)
    only((2,), all_side_backward)
    primal_two()
    only(((0, 1), (3, 0)), plane0)
    only((0, (3, 0)), core0)
    over_main(
        forward_two,
        [
            (backward_early, {2: list(range(NMAIN - EARLY, NMAIN))}),
            (operator_piece_late, {1: list(range(5))}),
            (side_backward, {(1, 1): [3]}),
            (plane0, {(1, 0): [3], (1, 1): [6], (2, 0): [1], (2, 1): [3], (3, 1): [0]}),
            (core0, {(1, 0): [4], (1, 1): [7], (2, 0): [2], (2, 1): [4], (3, 1): [1]}),
            (side_backward, {(1, 0): [5]}),
            (solved_at, {(2, 0): [4], (2, 1): [6], (3, 0): [2], (3, 1): [3]}),
            (sum1, {(2, 0): [7], (3, 0): [4], (3, 1): [6]}),
        ],
    )
    only(((1, 1),), side_backward_last)
    only((0, 1), solved_one)
    only(((1, 0),), side_backward_last)
    only((0,), all_side_backward)
    only((0, (1, 0)), sum1)
    only((0,), base_of_result)
    over_main(
        backward_late,
        [
            (sum1, {(1, 1): [1], (2, 1): [4]}),
            (plane1, {(0, 0): [1], (0, 1): [4], (1, 0): [3], (2, 0): [7]}),
            (core1, {(0, 0): [3], (0, 1): [5], (1, 0): [5]}),
        ],
    )
    only(((1, 1), (2, 1), 3), plane1)
    only((1, 2, 3), base_of_result)
    only(((1, 1), 2, 3), core1)
    for copies in (
        setup_z, setup_x, setup_c, ey, *coarse_p, *coarse_c, *fold_y, back_y[0],
    ):
        sent(copies)

    @pl.loop(0, NTURN)
    def _(i):
        @pl.when(k < SLABS - 1)
        def _():
            turned_up(i).wait_send()

        @pl.when(k > 0)
        def _():
            turned_down(i).wait_send()

    def sent_chunk(first):
        def step(sem, rows):
            @pl.when(k < SLABS - 1)
            def _():
                (f1_copy if first else f2_copy)(sem, rows).wait_send()

            @pl.when(k > 0)
            def _():
                (b1_copy if first else b2_copy)(sem, rows).wait_send()

        return step

    over_main(sent_chunk(True))
    over_side(sent_chunk(True))
    over_main(sent_chunk(False))

    out_ref[...] += n2[...]
    weights = jnp.concatenate([solved(1), jnp.zeros((EXTRA, RHS), F32)], axis=0).T
    factor = split(w0[...])
    half = RHS // 2
    stores = []
    for part in range(2):
        rows = pl.ds(part * half, half)
        out_ref[rows, :] += three(split(weights[part * half : part * half + half, 0:EXTRA]), factor, dot)
        stores.append(pltpu.make_async_copy(out_ref.at[rows], out_hbm.at[rows], out_s.at[part]))
        stores[-1].start()
    sent(back_y[1])
    for store in stores:
        store.wait()


def on_device(nz, nx, residual, inverse_slab, diagonal, primal_index, coarse_map, schur, basis_one, basis_two, cinv):
    blocks = nz * nx * 2
    dma = pltpu.SemaphoreType.DMA
    hbm = pl.BlockSpec(memory_space=pl.ANY)
    wide = lambda rows, kind=F32: pltpu.VMEM((rows, IFACE), kind)
    out = pl.pallas_call(
        functools.partial(kernel, nz, nx),
        out_shape=jax.ShapeDtypeStruct((RHS, IFACE), F32),
        in_specs=[hbm] * 9,
        out_specs=hbm,
        scratch_shapes=[
            wide(RHS),
            wide(1),
            *[pltpu.VMEM((1, PRIM), jnp.int32)] * 2,
            pltpu.VMEM((PRIM, PRIM), F32),
            wide(IFACE // blocks),
            wide(IFACE), wide(PRIM), wide(IFACE, BF16), wide(IFACE, BF16),
            *[wide(RHS + EXTRA)] * 5,
            *[wide(RHS)] * 5,
            wide(EXTRA),
            *[wide(PRIM)] * 5,
            wide(EXTRA, BF16),
            pltpu.VMEM((blocks, BLOCK, 128), F32),
            pltpu.VMEM((4, 8, 128), F32),
            pltpu.VMEM((8, PRIM, 128), F32),
            wide(EXTRA, BF16),
            *[pltpu.VMEM((128, blocks * 8), BF16)] * 2,
            *[pltpu.VMEM((2, 4, 8, 128), F32)] * 2,
            pltpu.VMEM((2, blocks, 8, 128), F32),
            pltpu.VMEM((2, 4, 16, 128), F32),
            pltpu.VMEM((EXTRA, RHS), F32),
            pltpu.VMEM((PRIM, RHS + EXTRA), F32),
            dma((PIECES + 8,)), dma((2,)),
            *[dma((NMAIN + NSIDE,))] * 4,
            *[dma((NMAIN,))] * 4,
            dma((2, NTURN)), dma((2, NTURN)),
            dma((nx,)), dma((nx,)), dma((nz,)), dma((nz,)), dma((2, nz * nx - 1)), dma((2, nz * nx - 1)), dma((3,)), dma((3,)),
            dma((5, SLABS)), dma((5, SLABS)), pltpu.SemaphoreType.REGULAR,
        ],
        compiler_params=pltpu.CompilerParams(
            collective_id=0, has_side_effects=True, vmem_limit_bytes=56 * 2**20
        ),
    )(
        residual[0, 0], inverse_slab[0, 0], basis_one[0, 0], basis_two[0, 0], diagonal[0], primal_index[0],
        coarse_map, schur[0], cinv.T,
    )
    return out[None, None]


def solution(mesh):
    nz, nx = 8, 4
    torus = Mesh(mesh.devices.reshape(nz, nx, 2, mesh.shape["slab"]), (*SUB, "slab"))
    in_specs = (
        P(SUB, "slab", None, None),
        P(SUB, "slab", None, None),
        P(SUB, "slab", None),
        P(SUB, "slab", None),
        P(SUB, None),
        P(SUB, None, None),
        P(SUB, "slab", None, None),
        P(SUB, "slab", None, None),
        P(None, SUB),
    )
    return jax.shard_map(
        functools.partial(on_device, nz, nx),
        mesh=torus,
        in_specs=in_specs,
        out_specs=P(SUB, "slab", None, None),
        check_vma=False,
    )
```

```python
import functools

import jax
import jax.numpy as jnp
from jax import lax
from jax.experimental import pallas as pl
from jax.experimental.pallas import tpu as pltpu
from jax.sharding import Mesh
from jax.sharding import PartitionSpec as P

SUB = ("z", "x", "core")
MESH = pl.DeviceIdType.MESH
F32 = jnp.float32
BF16 = jnp.bfloat16

RHS = 128
IFACE = 1024
PRIM = 32
EXTRA = 2 * PRIM
SLABS = 4
EARLY_Z = 3
LEADER = (5, 2)
MAIN = 16
SIDE = 32
NMAIN = RHS // MAIN
NTURN = PRIM // MAIN
EARLY = 3
NSIDE = EXTRA // SIDE
BLOCK = 40
PIECES = 8


def split(value):
    high = value.astype(BF16)
    return high, (value - high.astype(F32)).astype(BF16)


def dot(left, right):
    return jnp.dot(left, right, preferred_element_type=F32)


def dot_t(left, right):
    return lax.dot_general(left, right, (((1,), (1,)), ((), ())), preferred_element_type=F32)


def three(left, right, times):
    rows = left[0].shape[0]
    both = times(jnp.concatenate(left, axis=0), right[0])
    return both[:rows] + both[rows:] + times(left[0], right[1])


def dot3(left, right):
    return three(split(left), split(right), dot)


def column_of(row):
    eye = lax.broadcasted_iota(jnp.int32, (PRIM, PRIM), 0) == lax.broadcasted_iota(
        jnp.int32, (PRIM, PRIM), 1
    )
    return jnp.sum(jnp.where(eye, jnp.broadcast_to(row, (PRIM, PRIM)), 0.0), axis=1, keepdims=True)


def onehot_of(column, width):
    lanes = lax.broadcasted_iota(jnp.int32, (PRIM, width), 1).astype(F32)
    return jnp.where(lanes == column, 1.0, 0.0).astype(BF16)


def moved(tile, source, target):
    shift = 32 * (target - source) % 128
    return pltpu.roll(tile, shift, 1) if shift else tile


def groups_of(pieces):
    group = lax.broadcasted_iota(jnp.int32, (8, 128), 1) // 32
    total = jnp.zeros((8, 128), F32)
    for target, parts in enumerate(pieces):
        value = sum(moved(tile, source, target) for tile, source in parts)
        total = jnp.where(group == target, value, total)
    return total


def folded(tiles):
    return [groups_of([[(tiles[q], t)] for q in range(4)]) for t in range(4)]


def kernel(
    nz, nx,
    res_hbm, g_hbm, cb_hbm, cbas_hbm, diag_hbm, idx_hbm, map_hbm, schur_hbm, cinv_hbm, out_hbm,
    out_ref, diag_ref, idx_ref, map_ref, schur_ref, cinv_ref, g, cb, ghi, glo, vx, r1, f1, rb1, n1, x2, r2, f2, rb2, n2, w0,
    ta, tu, tr, tk, td, hot, gs, ms, es, eh, ch, cl, pf, ps, gp, ag, u1s, xys,
    in_s, out_s, f1_s, f1_r, b1_s, b1_r, f2_s, f2_r, b2_s, b2_r, t_s, t_r,
    gx_s, gx_r, gz_s, gz_r, gp_s, gp_r, gc_s, gc_r, y_s, y_r, ready,
):
    k = lax.axis_index("slab")
    z, x, core = lax.axis_index("z"), lax.axis_index("x"), lax.axis_index("core")
    blocks = 2 * nx * nz

    piece = IFACE // PIECES
    loads = [
        pltpu.make_async_copy(g_hbm.at[pl.ds(i * piece, piece)], g.at[pl.ds(i * piece, piece)], in_s.at[i])
        for i in range(PIECES)
    ]
    small = [
        pltpu.make_async_copy(src, dst, in_s.at[PIECES + 3 + i])
        for i, (src, dst) in enumerate(
            [(map_hbm, map_ref), (idx_hbm, idx_ref), (cinv_hbm, cinv_ref), (diag_hbm, diag_ref), (schur_hbm, schur_ref)]
        )
    ]
    load_res = pltpu.make_async_copy(res_hbm, vx.at[pl.ds(0, RHS)], in_s.at[PIECES])
    load_cb = pltpu.make_async_copy(cb_hbm, cb, in_s.at[PIECES + 1])
    load_cbas = pltpu.make_async_copy(cbas_hbm, w0.at[pl.ds(PRIM, PRIM)], in_s.at[PIECES + 2])
    for copy in (*small[:3], *loads, load_res, *small[3:], load_cb, load_cbas):
        copy.start()

    barrier = pltpu.get_barrier_semaphore()
    plane = [
        {"z": lax.rem(z + dz, nz), "x": lax.rem(x + dx, nx)}
        for dz in sorted(range(nz), key=lambda d: -min(d, nz - d))
        for dx in sorted(range(nx), key=lambda d: -min(d, nx - d))
        if dz or dx
    ]
    leads = (z == LEADER[0]) & (x == LEADER[1])

    def greet(other):
        pl.semaphore_signal(barrier, inc=1, device_id=other, device_id_type=MESH)

    for d in range(1, SLABS):
        greet({"slab": lax.rem(k + d, SLABS)})
    greet({"core": 1 - core})

    @pl.when(jnp.logical_not(leads))
    def _():
        greet({"z": LEADER[0], "x": LEADER[1]})

    own = (core * nx + x) * nz + z

    @pl.when(k == 0)
    def _():
        r1[...] = jnp.zeros_like(r1)
        tr[...] = jnp.zeros_like(tr)

    for copy in small[:3]:
        copy.wait()
    map_row = map_ref[...]
    map_col = column_of(map_row.astype(F32))
    owner, inner = map_row >> 4, map_row & 15
    place = (((owner & 1) * nx + ((owner >> 1) & 3)) * nz + (owner >> 3)) * 16 + inner
    hot[0:PRIM, :] = onehot_of(column_of(place.astype(F32)), IFACE)
    hot[PRIM:EXTRA, :] = onehot_of(column_of(idx_ref[...].astype(F32)), IFACE)

    quarter = pl.ds(pl.multiple_of(k * 256, 256), 256)
    gs[own, 0:16, :] = cinv_ref[:, quarter][:, 0:128]
    gs[own, 16:32, :] = cinv_ref[:, quarter][:, 128:256]
    lanes = lax.broadcasted_iota(jnp.int32, (PRIM, 128), 1)
    subl = lax.broadcasted_iota(jnp.int32, (PRIM, 128), 0)
    spread = jnp.where(lanes - 8 * lax.rem(own, 16) == subl % 8, jnp.broadcast_to(map_col, (PRIM, 128)), 0.0)
    for t in range(4):
        gs[own, 32 + t : 33 + t, :] = jnp.sum(spread[8 * t : 8 * t + 8], axis=0, keepdims=True)
    gs[own, 36:40, :] = jnp.zeros((4, 128), F32)

    def bases():
        for copy in (*small[3:], load_cb, load_cbas):
            copy.wait()
        w0[0:PRIM, :] = -dot3(schur_ref[...], cb[...])
        vx[RHS : RHS + EXTRA, :] = w0[...] * diag_ref[...]

    for i in range(PIECES):
        loads[i].wait()

        @pl.loop(0, piece // 64)
        def _(j):
            rows = pl.ds(pl.multiple_of(i * piece + j * 64, 64), 64)
            high, low = split(g[rows, :])
            ghi[rows, :] = high
            glo[rows, :] = low

    load_res.wait()
    pl.semaphore_wait(barrier, jnp.where(leads, SLABS + len(plane), SLABS))

    @pl.when(leads)
    def _():
        for other in plane:
            pl.semaphore_signal(ready, inc=1, device_id=other, device_id_type=MESH)

    def plane_ready():
        @pl.when(jnp.logical_not(leads))
        def _():
            pl.semaphore_wait(ready, 1)

        start(setup_z)


    def remote(src, dst, send, recv, to):
        return pltpu.make_async_remote_copy(
            src_ref=src, dst_ref=dst, send_sem=send, recv_sem=recv, device_id=to, device_id_type=MESH
        )

    up = {"slab": lax.rem(k + 1, SLABS)}
    down = {"slab": lax.rem(k + SLABS - 1, SLABS)}

    def together(copies, whole, send, recv):
        return copies, remote(whole, whole, send, recv, down)

    def gather_z(buf):
        copies = [
            remote(buf.at[own], buf.at[own], gz_s.at[0], gz_r.at[0], {"z": lax.rem(z + d, nz)}) for d in range(1, nz)
        ]
        return together(copies, buf.at[pl.ds(0, nz - 1)], gz_s.at[0], gz_r.at[0])

    def gather_x(buf):
        part = pl.ds((core * nx + x) * nz, nz)
        copies = [
            remote(buf.at[part], buf.at[part], gx_s.at[0], gx_r.at[0], {"x": lax.rem(x + d, nx)}) for d in range(1, nx)
        ]
        return together(copies, buf.at[pl.ds(0, (nx - 1) * nz)], gx_s.at[0], gx_r.at[0])

    def gather_plane(buf, n):
        copies = [remote(buf.at[own], buf.at[own], gp_s.at[n], gp_r.at[n], other) for other in plane]
        return together(copies, buf.at[pl.ds(0, len(plane))], gp_s.at[n], gp_r.at[n])

    def gather_core(buf, n):
        part = pl.ds(core * nx * nz, nx * nz)
        copies = [remote(buf.at[part], buf.at[part], gc_s.at[n], gc_r.at[n], {"core": 1 - core})]
        return together(copies, buf.at[part], gc_s.at[n], gc_r.at[n])

    def to_slabs(copy_of, whole, n):
        copies = []
        for d in range(1, SLABS):
            other = lax.rem(k + d, SLABS)
            src, dst = copy_of(other)
            copies.append(remote(src, dst, y_s.at[n], y_r.at[n], {"slab": other}))
        return together(copies, whole, y_s.at[n], y_r.at[n])

    def start(group):
        for copy in group[0]:
            copy.start()

    def arrived(group):
        group[1].wait_recv()

    def sent(group):
        group[1].wait_send()

    setup_z, setup_x, setup_c = gather_z(gs), gather_x(gs), gather_core(gs, 2)
    e_part = pl.ds(2 * k, 2)
    ey = to_slabs(lambda other: (es.at[e_part], es.at[e_part]), es.at[pl.ds(0, 6)], 4)
    coarse_p = [gather_plane(gp.at[n], n) for n in range(2)]
    coarse_c = [gather_core(gp.at[n], n) for n in range(2)]
    fold_y = [to_slabs(lambda other: (pf.at[n, other], ps.at[n, k]), ps.at[n, pl.ds(0, 3)], 2 * n) for n in range(2)]
    back_y = [to_slabs(lambda other: (ag.at[n, k], ag.at[n, k]), ag.at[n, pl.ds(0, 3)], 2 * n + 1) for n in range(2)]

    def times_g(value):
        return three(split(value), (ghi[...], glo[...]), dot)

    def times_g_turned(value):
        return three(split(value), (ghi[...], glo[...]), dot_t)

    def main_chunk(i):
        return i, pl.ds(pl.multiple_of(i * MAIN, MAIN), MAIN)

    def side_chunk(i):
        return NMAIN + i, pl.ds(pl.multiple_of(RHS + i * SIDE, SIDE), SIDE)

    def f1_copy(sem, rows):
        return remote(f1.at[rows], r1.at[rows], f1_s.at[0], f1_r.at[sem], up)

    def b1_copy(sem, rows):
        return remote(n1.at[rows], rb1.at[rows], b1_s.at[0], b1_r.at[sem], down)

    def f2_copy(sem, rows):
        return remote(f2.at[rows], r2.at[rows], f2_s.at[0], f2_r.at[sem], up)

    def b2_copy(sem, rows):
        return remote(n2.at[rows], rb2.at[rows], b2_s.at[0], b2_r.at[sem], down)

    def forward_one(sem, rows):
        @pl.when(k > 0)
        def _():
            f1_copy(sem, rows).wait_recv()

        value = times_g(vx[rows, :] + r1[rows, :])
        f1[rows, :] = value

        @pl.when(k < SLABS - 1)
        def _():
            f1_copy(sem, rows).start()

        @pl.when(k == SLABS - 1)
        def _():
            n1[rows, :] = value
            b1_copy(sem, rows).start()

    def backward_one(sem, rows):
        @pl.when(k < SLABS - 1)
        def _():
            b1_copy(sem, rows).wait_recv()
            n1[rows, :] = f1[rows, :] + times_g(rb1[rows, :])

            @pl.when(k > 0)
            def _():
                b1_copy(sem, rows).start()

    def between(sem, rows):
        backward_one(sem, rows)
        value = vx[rows, :] - diag_ref[...] * n1[rows, :]
        x2[rows, :] = value

        @pl.when(k == 0)
        def _():
            f2[rows, :] = times_g(value)
            f2_copy(sem, rows).start()

    def forward_two(sem, rows):
        @pl.when(k > 0)
        def _():
            f2_copy(sem, rows).wait_recv()
            value = times_g(x2[rows, :] + r2[rows, :])
            f2[rows, :] = value

            @pl.when(k < SLABS - 1)
            def _():
                f2_copy(sem, rows).start()

            @pl.when(k == SLABS - 1)
            def _():
                n2[rows, :] = value
                b2_copy(sem, rows).start()

    def backward_two(sem, rows):
        @pl.when(k < SLABS - 1)
        def _():
            b2_copy(sem, rows).wait_recv()
            n2[rows, :] = f2[rows, :] + times_g(rb2[rows, :])

            @pl.when(k > 0)
            def _():
                b2_copy(sem, rows).start()

    early = z < EARLY_Z

    def here(who):
        if isinstance(who, int):
            return k == who
        return (k == who[0]) & (early if who[1] else jnp.logical_not(early))

    def over_main(step, hooks=()):
        @pl.loop(0, NMAIN)
        def _(i):
            step(*main_chunk(i))
            for act, places in hooks:
                spots = [(here(who), at) for who, chunks in places.items() for at in chunks]
                due = functools.reduce(jnp.logical_or, [mine & (i == at) for mine, at in spots])
                done = sum(jnp.where(mine & (i > at), 1, 0) for mine, at in spots)

                @pl.when(due)
                def _():
                    act(done)

    def over_side(step):
        @pl.loop(0, NSIDE)
        def _(i):
            step(*side_chunk(i))

    def only(those, *acts):
        @pl.when(functools.reduce(jnp.logical_or, [here(who) for who in those]))
        def _():
            for act in acts:
                act()

    def once(act, *args):
        return lambda *_: act(*args)

    def side_forward(i):
        forward_one(*side_chunk(i))

    def side_backward(i):
        backward_one(*side_chunk(i))

    def all_side_forward():
        over_side(forward_one)

    def all_side_backward():
        over_side(backward_one)

    def turned_up(i):
        rows = pl.ds(pl.multiple_of(i * MAIN, MAIN), MAIN)
        return remote(tu.at[rows], tr.at[rows], t_s.at[0], t_r.at[0, i], up)

    def turned_down(i):
        rows = pl.ds(pl.multiple_of(i * MAIN, MAIN), MAIN)
        return remote(tk.at[rows], td.at[rows], t_s.at[1], t_r.at[1, i], down)

    def adjoint_up(i):
        rows = pl.ds(pl.multiple_of(i * MAIN, MAIN), MAIN)

        @pl.when(k > 0)
        def _():
            turned_up(i).wait_recv()

        value = hot[pl.ds(pl.multiple_of(PRIM + i * MAIN, MAIN), MAIN), :].astype(F32) + tr[rows, :]
        ta[rows, :] = value
        result = times_g_turned(value)

        @pl.when(k < SLABS - 1)
        def _():
            tu[rows, :] = result
            turned_up(i).start()

        @pl.when(k == SLABS - 1)
        def _():
            tk[rows, :] = result
            turned_down(i).start()

    def adjoint_down(i):
        rows = pl.ds(pl.multiple_of(i * MAIN, MAIN), MAIN)
        turned_down(i).wait_recv()
        tk[rows, :] = times_g_turned(ta[rows, :] + td[rows, :])

        @pl.when(k > 0)
        def _():
            turned_down(i).start()

    def setup_z_in():
        arrived(setup_z)
        start(setup_x)

    def setup_x_in():
        arrived(setup_x)
        start(setup_c)

    def setup_core_in():
        arrived(setup_c)
        for half in range(2):
            high, low = split(gs[:, 16 * half : 16 * half + 16, :].reshape(IFACE, 128))
            es[2 * k + half] = dot(hot[0:PRIM, :], high) + dot(hot[0:PRIM, :], low)
        start(ey)

    def operator_base():
        arrived(ey)
        for a in range(4):
            ms[a] = jnp.sum(gs[16 * a : 16 * a + 16, 32:40, :], axis=0)
        wide = jnp.concatenate([es[b] for b in range(8)], axis=1)
        eh[...] = jnp.concatenate(split(wide), axis=0)

    def operator_piece(i):
        t, half = i // 2, i % 2
        depth = lax.broadcasted_iota(jnp.int32, (IFACE, 256), 0).astype(F32)
        wanted = jnp.concatenate([ms[2 * half, pl.ds(t, 1), :], ms[2 * half + 1, pl.ds(t, 1), :]], axis=1)
        both = dot(eh[...], jnp.where(depth == wanted, 1.0, 0.0).astype(BF16))
        high, low = split(both[0:PRIM] + both[PRIM:])
        rows, columns = pl.ds(pl.multiple_of(t * PRIM, PRIM), PRIM), pl.ds(pl.multiple_of(half * 256, 256), 256)
        ch[rows, columns] = high
        cl[rows, columns] = low

    def coarse_operator():
        operator_base()

        @pl.loop(0, 8)
        def _(i):
            operator_piece(i)

    def give_primal(n, primal):
        tiles = folded([primal[8 * t : 8 * t + 8] for t in range(4)])
        for q in range(4):
            pf[n, q] = tiles[q]
        ps[n, k] = pf[n, k]
        start(fold_y[n])

    def primal_one():
        turned = split(tk[...])
        give_primal(0, three(turned, split(vx[0:RHS, :]), dot_t))

    def solve_sum(n):
        arrived(fold_y[n])
        total = jnp.sum(ps[n], axis=0)
        gp[n, own] = total
        ag[n, k, 0:8, :] = total
        start(coarse_p[n])

    def solve_plane(n):
        arrived(coarse_p[n])
        start(coarse_c[n])

    def solve_core(n):
        arrived(coarse_c[n])
        everyone = split(gp[n].reshape(blocks * 8, 128))
        product = three((ch[...], cl[...]), everyone, dot)
        ag[n, k, 8:16, :] = groups_of(
            [[(product[32 * t + 8 * target : 32 * t + 8 * target + 8], t) for t in range(4)] for target in range(4)]
        )
        start(back_y[n])

    def solved(n):
        arrived(back_y[n])
        tiles = [ag[n, q] for q in range(4)]
        return jnp.concatenate(
            [*folded([tile[0:8] for tile in tiles]), *folded([tile[8:16] for tile in tiles])], axis=0
        )

    def primal_two():
        turned = split(tk[...])
        xys[:, 0:RHS] = three(turned, split(x2[...]), dot_t)
        xys[:, RHS : RHS + EXTRA] = three(turned, split(vx[RHS : RHS + EXTRA, :]), dot_t)

    def solved_one():
        u1 = solved(0)
        u1s[...] = u1
        give_primal(1, xys[:, 0:RHS] - dot3(xys[:, RHS : RHS + EXTRA], u1))

    def base_of_result():
        u1 = u1s[...]
        weights = jnp.concatenate([u1, u1], axis=0).T
        base = jnp.concatenate([-n1[RHS : RHS + EXTRA, :], w0[...]], axis=0)
        out_ref[...] = n1[0:RHS, :] + dot3(weights, base)

    sum0, plane0, core0 = (once(act, 0) for act in (solve_sum, solve_plane, solve_core))
    sum1, plane1, core1 = (once(act, 1) for act in (solve_sum, solve_plane, solve_core))
    setup_z_at, setup_x_at, setup_core_at = map(once, (setup_z_in, setup_x_in, setup_core_in))
    primal_at, solved_at, ready_at = once(primal_one), once(solved_one), once(plane_ready)

    def side_backward_last():
        side_backward(NSIDE - 1)

    def operator_piece_late(i):
        operator_piece(3 + i)

    def backward_early(i):
        backward_two(*main_chunk(i))

    def backward_late(sem, rows):
        @pl.when((k != 2) | (sem >= EARLY))
        def _():
            backward_two(sem, rows)

    only((1, 2, 3), bases)
    only(((1, 0), 2, 3), plane_ready)
    only(((2, 0), (3, 0)), setup_z_in)

    @pl.loop(0, NTURN)
    def _(i):
        adjoint_up(i)

    only(((3, 1),), setup_z_in)
    over_main(
        forward_one,
        [
            (ready_at, {(0, 0): [1], (1, 1): [1]}),
            (setup_z_at, {(1, 0): [4], (1, 1): [5], (2, 1): [3]}),
            (setup_x_at, {(2, 0): [4], (3, 0): [0], (3, 1): [6]}),
            (setup_core_at, {(2, 0): [6], (3, 0): [2], (3, 1): [7]}),
            (adjoint_down, {2: [5, 6]}),
        ],
    )
    only(((0, 1),), plane_ready)
    only((0,), bases, all_side_forward, setup_z_in, setup_x_in, setup_core_in)
    only((1,), all_side_forward, setup_x_in)
    @pl.when(k < 2)
    def _():
        @pl.loop(0, NTURN)
        def _(i):
            adjoint_down(i)
            pl.when(here((1, 0)) & (i == 0))(setup_core_in)

    only((0, 3), primal_one)
    over_main(
        between,
        [
            (primal_at, {1: [1], 2: [2]}),
            (setup_x_at, {(2, 1): [1]}),
            (setup_core_at, {(1, 1): [0], (2, 1): [3]}),
            (once(operator_base), {1: [5]}),
            (operator_piece, {1: [5, 6, 7]}),
            (side_forward, {2: [4, 6]}),
            (sum0, {0: [1], 1: [6]}),
            (plane0, {(0, 0): [6]}),
        ],
    )
    only((0,), coarse_operator)
    only((3,), all_side_forward)
    only((2, 3), sum0, coarse_operator)
    only((2,), all_side_backward)
    primal_two()
    only(((0, 1), (3, 0)), plane0)
    only((0, (3, 0)), core0)
    over_main(
        forward_two,
        [
            (backward_early, {2: list(range(NMAIN - EARLY, NMAIN))}),
            (operator_piece_late, {1: list(range(5))}),
            (side_backward, {(1, 1): [3]}),
            (plane0, {(1, 0): [3], (1, 1): [6], (2, 0): [1], (2, 1): [3], (3, 1): [0]}),
            (core0, {(1, 0): [4], (1, 1): [7], (2, 0): [2], (2, 1): [4], (3, 1): [1]}),
            (side_backward, {(1, 0): [5]}),
            (solved_at, {(2, 0): [4], (2, 1): [6], (3, 0): [2], (3, 1): [3]}),
            (sum1, {(2, 0): [7], (3, 0): [4], (3, 1): [6]}),
        ],
    )
    only(((1, 1),), side_backward_last)
    only((0, 1), solved_one)
    only(((1, 0),), side_backward_last)
    only((0,), all_side_backward)
    only((0, (1, 0)), sum1)
    only((0,), base_of_result)
    over_main(
        backward_late,
        [
            (sum1, {(1, 1): [1], (2, 1): [4]}),
            (plane1, {(0, 0): [1], (0, 1): [4], (1, 0): [3], (2, 0): [7]}),
            (core1, {(0, 0): [3], (0, 1): [5], (1, 0): [5]}),
        ],
    )
    only(((1, 1), (2, 1), 3), plane1)
    only((1, 2, 3), base_of_result)
    only(((1, 1), 2, 3), core1)
    for group in (
        setup_z, setup_x, setup_c, ey, *coarse_p, *coarse_c, *fold_y, back_y[0],
    ):
        sent(group)

    @pl.when(k < SLABS - 1)
    def _():
        for src, dst, send, recv in ((tu, tr, t_s.at[0], t_r.at[0, 0]), (f1, r1, f1_s.at[0], f1_r.at[0]), (f2, r2, f2_s.at[0], f2_r.at[0])):
            remote(src, dst, send, recv, up).wait_send()

    @pl.when(k > 0)
    def _():
        for src, dst, send, recv in ((tk, td, t_s.at[1], t_r.at[1, 0]), (n1, rb1, b1_s.at[0], b1_r.at[0]), (n2, rb2, b2_s.at[0], b2_r.at[0])):
            remote(src, dst, send, recv, down).wait_send()

    out_ref[...] += n2[...]
    weights = jnp.concatenate([solved(1), jnp.zeros((EXTRA, RHS), F32)], axis=0).T
    factor = split(w0[...])
    half = RHS // 2
    stores = []
    for part in range(2):
        rows = pl.ds(part * half, half)
        out_ref[rows, :] += three(split(weights[part * half : part * half + half, 0:EXTRA]), factor, dot)
        stores.append(pltpu.make_async_copy(out_ref.at[rows], out_hbm.at[rows], out_s.at[part]))
        stores[-1].start()
    sent(back_y[1])
    for store in stores:
        store.wait()


def on_device(nz, nx, residual, inverse_slab, diagonal, primal_index, coarse_map, schur, basis_one, basis_two, cinv):
    blocks = nz * nx * 2
    dma = pltpu.SemaphoreType.DMA
    hbm = pl.BlockSpec(memory_space=pl.ANY)
    wide = lambda rows, kind=F32: pltpu.VMEM((rows, IFACE), kind)
    out = pl.pallas_call(
        functools.partial(kernel, nz, nx),
        out_shape=jax.ShapeDtypeStruct((RHS, IFACE), F32),
        in_specs=[hbm] * 9,
        out_specs=hbm,
        scratch_shapes=[
            wide(RHS),
            wide(1),
            *[pltpu.VMEM((1, PRIM), jnp.int32)] * 2,
            pltpu.VMEM((PRIM, PRIM), F32),
            wide(IFACE // blocks),
            wide(IFACE), wide(PRIM), wide(IFACE, BF16), wide(IFACE, BF16),
            *[wide(RHS + EXTRA)] * 5,
            *[wide(RHS)] * 5,
            wide(EXTRA),
            *[wide(PRIM)] * 5,
            wide(EXTRA, BF16),
            pltpu.VMEM((blocks, BLOCK, 128), F32),
            pltpu.VMEM((4, 8, 128), F32),
            pltpu.VMEM((8, PRIM, 128), F32),
            wide(EXTRA, BF16),
            *[pltpu.VMEM((128, blocks * 8), BF16)] * 2,
            *[pltpu.VMEM((2, 4, 8, 128), F32)] * 2,
            pltpu.VMEM((2, blocks, 8, 128), F32),
            pltpu.VMEM((2, 4, 16, 128), F32),
            pltpu.VMEM((EXTRA, RHS), F32),
            pltpu.VMEM((PRIM, RHS + EXTRA), F32),
            dma((PIECES + 8,)), dma((2,)),
            *[dma((1,)), dma((NMAIN + NSIDE,))] * 2,
            *[dma((1,)), dma((NMAIN,))] * 2,
            dma((2,)), dma((2, NTURN)),
            *[dma((1,))] * 4, *[dma((2,))] * 2, *[dma((3,))] * 2,
            dma((5,)), dma((5,)), pltpu.SemaphoreType.REGULAR,
        ],
        compiler_params=pltpu.CompilerParams(
            collective_id=0, has_side_effects=True, vmem_limit_bytes=56 * 2**20
        ),
    )(
        residual[0, 0], inverse_slab[0, 0], basis_one[0, 0], basis_two[0, 0], diagonal[0], primal_index[0],
        coarse_map, schur[0], cinv.T,
    )
    return out[None, None]


def solution(mesh):
    nz, nx = 8, 4
    torus = Mesh(mesh.devices.reshape(nz, nx, 2, mesh.shape["slab"]), (*SUB, "slab"))
    in_specs = (
        P(SUB, "slab", None, None),
        P(SUB, "slab", None, None),
        P(SUB, "slab", None),
        P(SUB, "slab", None),
        P(SUB, None),
        P(SUB, None, None),
        P(SUB, "slab", None, None),
        P(SUB, "slab", None, None),
        P(None, SUB),
    )
    return jax.shard_map(
        functools.partial(on_device, nz, nx),
        mesh=torus,
        in_specs=in_specs,
        out_specs=P(SUB, "slab", None, None),
        check_vma=False,
    )
```
